128 devices in a mesh: ctx: 8 (over z, x_lo), tp: 4 (over x_hi, core), dp: 4 (over y).
Axes of the slice: x: 4 (x_hi: 2, x_lo: 2; x = x_hi * 2 + x_lo), y: 4, z: 4, core: 2. Of those that a mesh axis runs over, the one named last changes fastest.
Arguments:
- hidden: bfloat16 [4, 4096, 4096], P('dp', 'ctx', 'tp'), may hold values from -6 to 6
- target: bfloat16 [4, 4096, 4096], P('dp', 'ctx', 'tp'), may hold values from -24 to 24
- gain: float32 [4096], replicated, may hold values from 0.5 to 1.5
- w_query: bfloat16 [4096, 2048], P(('ctx', 'dp'), 'tp'), may hold values from -2.15625 to 2.15625
- w_key: bfloat16 [4096, 512], P(('ctx', 'dp'), 'tp'), may hold values from -0.09375 to 0.09375
- value_matrix: bfloat16 [4096, 512], P(('ctx', 'dp'), 'tp'), may hold values from -0.09375 to 0.09375
- w_out: bfloat16 [2048, 4096], P('tp', ('ctx', 'dp')), may hold values from -0.125 to 0.125
- block_order: int32 [16], replicated, may hold values from 0 to 15, each once
Outputs:
- branch: bfloat16 [4, 4096, 4096], P('dp', 'ctx', 'tp')
- loss: float32 [], replicated
The draws below stay inside these ranges and needn't reach their ends.
Inputs may be any that keep to these rules, and one draw needn't show every extreme that they name: block_order is a permutation of 0 to 15.
All inputs are finite; a program needn't handle non-finite values.
Results may differ from the reference program's by a relative error of at most 0.013.
The reference program's roundings to bfloat16 on the way (of `normed` and `attn`) count: a program that leaves them out, or rounds other values in their place, can miss the bound.
Values may be sent and summed in bfloat16 or wider, within the bound.
A program may use at most 128 MiB of HBM per device.

```python
import math
import jax
import jax.numpy as jnp
from jax import lax

MODEL_WIDTH = 4096
QUERY_HEADS = 16
KEY_VALUE_HEADS = 4
HEAD_SIZE = 128
CH = 256
SEQUENCE_LENGTH = 4096
SEQS = 4
N_CTX = 8
N_TP = 4


def key_weights(key):
    random_jitter = jax.random.normal(jax.random.fold_in(key, 11), (MODEL_WIDTH, KEY_VALUE_HEADS * HEAD_SIZE), jnp.float32)
    return jnp.clip(random_jitter, -6.0, 6.0) / MODEL_WIDTH ** 0.5


def draw_w_key(key, part):
    return key_weights(key).astype(jnp.bfloat16)


def draw_w_query(key, part):
    random_jitter = jax.random.normal(jax.random.fold_in(key, 23), (MODEL_WIDTH, QUERY_HEADS * HEAD_SIZE), jnp.float32)
    base = jnp.clip(random_jitter, -6.0, 6.0) * (3.0 / MODEL_WIDTH ** 0.5)
    return base.astype(jnp.bfloat16)


def draw_hidden(key, part):
    base = jnp.clip(jax.random.normal(jax.random.fold_in(key, 41), (SEQS, SEQUENCE_LENGTH, MODEL_WIDTH), jnp.float32), -6.0, 6.0)
    return base.astype(jnp.bfloat16)


def draw_target(key, part):
    fraction = jnp.arange(SEQUENCE_LENGTH, dtype=jnp.float32) / (SEQUENCE_LENGTH - 1)
    scale = jnp.exp(fraction * jnp.log(6.0))
    noise = jnp.clip(jax.random.normal(jax.random.fold_in(key, 67), (SEQS, SEQUENCE_LENGTH, MODEL_WIDTH), jnp.float32), -4.0, 4.0)
    return jnp.clip(noise * scale[None, :, None], -24.0, 24.0).astype(jnp.bfloat16)


def shard_levels(rng, extent, cuts, least, largest):
    def one(dim, shards_of):
        steps = jax.random.uniform(jax.random.fold_in(jax.random.fold_in(rng, 6), dim), (shards_of,), jnp.float32, least / len(cuts), largest / len(cuts))
        return jnp.repeat(jnp.exp(steps), extent[dim] // shards_of).reshape((-1,) + (1,) * (len(extent) - dim - 1))

    factor_of = one(*cuts[0])
    for cut in cuts[1:]:
        factor_of = factor_of * one(*cut)
    return factor_of


def normal_values(own_key, extent, scale, bound, shards=(), kind=jnp.bfloat16):
    values = scale * jax.random.normal(own_key, extent, jnp.float32)
    if shards:
        values = values * shard_levels(own_key, extent, shards, -0.22, 0.18)
    return jnp.clip(values, -bound, bound).astype(kind)


def setup_inputs(seed: int = 0) -> dict:
    seeds = jax.random.split(jax.random.key(seed), 9)
    hidden = draw_hidden(jax.random.fold_in(seeds[8], 71), 0)
    target = draw_target(jax.random.fold_in(seeds[8], 71), 0)
    gain = jnp.clip(1.0 + 0.1 * jax.random.normal(seeds[2], (MODEL_WIDTH,), jnp.float32), 0.5, 1.5)
    w_query = draw_w_query(jax.random.fold_in(seeds[8], 71), 0)
    w_key = draw_w_key(jax.random.fold_in(seeds[8], 71), 0)
    value_matrix = normal_values(seeds[5], (MODEL_WIDTH, KEY_VALUE_HEADS * HEAD_SIZE), MODEL_WIDTH ** -0.5, 0.09375, ((0, 32), (1, 4)))
    w_out = normal_values(seeds[6], (QUERY_HEADS * HEAD_SIZE, MODEL_WIDTH), (QUERY_HEADS * HEAD_SIZE) ** -0.5, 0.125, ((0, 4), (1, 32)))
    block_order = jax.random.permutation(seeds[7], 2 * N_CTX).astype(jnp.int32)
    return {"hidden": hidden, "target": target, "gain": gain, "w_query": w_query, "w_key": w_key, "value_matrix": value_matrix, "w_out": w_out, "block_order": block_order}


rope_base = 500000.0

def apply_rotary(values, token_places):
    half = values.shape[-1] // 2
    freqs = rope_base ** (-(jnp.arange(half, dtype=jnp.float32) * 2.0) / values.shape[-1])
    angles = token_places.astype(jnp.float32)[:, None] * freqs[None, :]
    cosine = jnp.cos(angles)[:, None, :]
    sine = jnp.sin(angles)[:, None, :]
    first = values[..., :half]
    second = values[..., half:]
    return jnp.concatenate([first * cosine - second * sine, second * cosine + first * sine], axis=-1)

def one_sequence(states, gain, w_query, w_key, value_matrix, w_out, token_places):
    query_group = QUERY_HEADS // KEY_VALUE_HEADS
    wide = states.astype(jnp.float32)
    normed = (wide * lax.rsqrt(lax.optimization_barrier(jnp.mean(wide * wide, axis=1, keepdims=True)) + 1e-05) * gain[None, :]).astype(jnp.bfloat16)
    query_rows = jnp.dot(normed, w_query, preferred_element_type=jnp.float32)
    key = jnp.dot(normed, w_key, preferred_element_type=jnp.float32)
    value_rows = jnp.dot(normed, value_matrix, preferred_element_type=jnp.float32)
    query_rows = apply_rotary(query_rows.reshape(SEQUENCE_LENGTH, QUERY_HEADS, HEAD_SIZE), token_places).astype(jnp.bfloat16).reshape(SEQUENCE_LENGTH, KEY_VALUE_HEADS, query_group, HEAD_SIZE)
    key = apply_rotary(key.reshape(SEQUENCE_LENGTH, KEY_VALUE_HEADS, HEAD_SIZE), token_places).astype(jnp.bfloat16)
    value_rows = value_rows.astype(jnp.bfloat16).reshape(SEQUENCE_LENGTH, KEY_VALUE_HEADS, HEAD_SIZE)
    scale = 1.0 / HEAD_SIZE ** 0.5
    block_rows = math.gcd(SEQUENCE_LENGTH, 1024)

    def head_split(index):
        qhead = lax.dynamic_index_in_dim(query_rows, index, 1, False)
        khead = lax.dynamic_index_in_dim(key, index, 1, False).astype(jnp.float32)
        vhead = lax.dynamic_index_in_dim(value_rows, index, 1, False).astype(jnp.float32)

        def per_block(number):
            first_row = (number * block_rows).astype(jnp.int32)
            qpart = lax.dynamic_slice_in_dim(qhead, first_row, block_rows, 0).astype(jnp.float32)
            qplaces = lax.dynamic_slice_in_dim(token_places, first_row, block_rows, 0)
            allowed = qplaces[:, None] >= token_places[None, :]
            scores = jnp.einsum('qgd,kd->gqk', qpart, khead) * scale
            scores = jnp.where(allowed[None], scores, -1e+30)
            peak = lax.optimization_barrier(jnp.max(scores, axis=-1, keepdims=True))
            weights = jnp.where(allowed[None], jnp.exp(scores - peak), 0.0)
            total = lax.optimization_barrier(jnp.sum(weights, axis=-1))
            rounded = weights.astype(jnp.bfloat16).astype(jnp.float32)
            mixed = jnp.einsum('gqk,kd->qgd', rounded, vhead)
            return (mixed / jnp.transpose(total)[:, :, None]).astype(jnp.bfloat16)
        pieces = lax.map(per_block, jnp.arange(SEQUENCE_LENGTH // block_rows, dtype=jnp.int32))
        return pieces.reshape(SEQUENCE_LENGTH, query_group, HEAD_SIZE)
    head_list = lax.map(head_split, jnp.arange(KEY_VALUE_HEADS, dtype=jnp.int32))
    attn = jnp.transpose(head_list, (1, 0, 2, 3)).reshape(SEQUENCE_LENGTH, QUERY_HEADS * HEAD_SIZE)
    width = QUERY_HEADS * HEAD_SIZE // N_TP
    summed = jnp.zeros((SEQUENCE_LENGTH, MODEL_WIDTH), jnp.float32)
    for part in range(N_TP):
        partial_term = jnp.dot(attn[:, part * width:(part + 1) * width], w_out[part * width:(part + 1) * width], preferred_element_type=jnp.float32)
        summed = summed + partial_term.astype(jnp.bfloat16).astype(jnp.float32)
    return summed.astype(jnp.bfloat16)

def reference(hidden, target, gain, w_query, w_key, value_matrix, w_out, block_order):
    rows = jnp.arange(SEQUENCE_LENGTH, dtype=jnp.int32)
    token_places = (jnp.take(block_order, rows // CH).astype(jnp.int32) * CH + rows % CH).astype(jnp.int32)
    outputs = []
    squares = jnp.zeros((), jnp.float32)
    for index in range(SEQS):
        result = one_sequence(hidden[index], gain, w_query, w_key, value_matrix, w_out, token_places)
        outputs.append(result)
        resid = hidden[index].astype(jnp.float32) + result.astype(jnp.float32) - target[index].astype(jnp.float32)
        squares = squares + jnp.sum(resid * resid)
    loss = squares / (SEQS * SEQUENCE_LENGTH * MODEL_WIDTH)
    return (jnp.stack(outputs), loss)
```

```python
import types

import jax
import jax.numpy as jnp
from jax import lax
from jax.experimental import pallas as pl
from jax.experimental.pallas import tpu as pltpu
from jax.sharding import PartitionSpec as P

MODEL_WIDTH = 4096
QUERY_HEADS = 16
KEY_VALUE_HEADS = 4
HEAD_SIZE = 128
TP = "tp"
CTX_DP = ("ctx", "dp")
CTX = "ctx"
CTX_TP_DP = ("ctx", "tp", "dp")


rope_base = 500000.0


def side_by_side(arrays, axis, dim, along):
    widths = [a.shape[along] for a in arrays]
    both = jnp.concatenate(arrays, axis=along)
    whole = lax.all_gather(both, axis, axis=dim, tiled=True)
    return tuple(jnp.split(whole, [sum(widths[:k]) for k in range(1, len(widths))], axis=along))


def shifted(value, axis, by):
    peers = lax.axis_size(axis)
    return lax.ppermute(value, axis, [(i, (i + by) % peers) for i in range(peers)])


def by_axis(value, axes):
    for axis in axes:
        value = lax.psum(value, axis)
    return value


def positions(order, start, rows, half):
    index = start + lax.iota(jnp.int32, rows)
    block = index // half
    slots = lax.iota(jnp.int32, order.shape[0])
    chosen = jnp.sum(jnp.where(block[:, None] == slots[None, :], order[None, :], 0), axis=1)
    return chosen * half + index % half


def apply_rotary(values, token_places):
    half = values.shape[-1] // 2
    freqs = rope_base ** (-(jnp.arange(half, dtype=jnp.float32) * 2.0) / values.shape[-1])
    angles = token_places.astype(jnp.float32)[:, None] * freqs[None, :]
    cosine = jnp.cos(angles)[:, None, :]
    sine = jnp.sin(angles)[:, None, :]
    first = values[..., :half]
    second = values[..., half:]
    return jnp.concatenate(
        [first * cosine - second * sine, second * cosine + first * sine], axis=-1
    )


MESH = pl.DeviceIdType.MESH
SIDES = (1, -1)


def here():
    c, t, d = lax.axis_index("ctx"), lax.axis_index("tp"), lax.axis_index("dp")
    return c, t, d


class Net:
    def __init__(self, send_sems, recv_sems):
        self.send_sems, self.recv_sems = send_sems, recv_sems
        self.started = []

    def copy(self, k, src, dst, dev):
        c, t, d = dev
        return pltpu.make_async_remote_copy(
            src_ref=src,
            dst_ref=dst,
            send_sem=self.send_sems.at[k],
            recv_sem=self.recv_sems.at[k],
            device_id=(c, t, d),
            device_id_type=MESH,
        )

    def send(self, ref, dev, dst=None):
        k = len(self.started)
        copy = self.copy(k, ref, ref if dst is None else dst, dev)
        copy.start()
        self.started.append((copy, dev))
        return k

    def recv(self, k, ref):
        self.copy(k, ref, ref, self.started[k][1]).wait_recv()

    def finish(self):
        for copy, _ in self.started:
            copy.wait_send()


def places():
    c, t, d = here()
    z, xl = c // 2, c % 2
    c1 = c + 1 - 2 * xl
    t1 = t + 1 - 2 * (t % 2)
    t2 = (t + 2) % 4
    t3 = (t1 + 2) % 4
    return types.SimpleNamespace(
        c=c, t=t, d=d, z=z, xl=xl, xo=1 - xl, c1=c1, t1=t1, t2=t2, t3=t3,
        P=(c1, t, d), Q=(c1, t2, d), C=(c, t1, d), R=(c, t2, d), D=(c, t3, d),
        Y={s: (c, t, (d + s) % 4) for s in SIDES},
        Z={s: ((c + 2 * s) % 8, t, d) for s in SIDES},
        yo={s: (d - s) % 4 for s in SIDES},
        zo={s: (z - s) % 4 for s in SIDES},
        y2=(d + 2) % 4, z2=(z + 2) % 4,
    )


def greet(m):
    barrier = pltpu.get_barrier_semaphore()
    others = [m.P, m.Q, m.C, m.R, m.D, m.Y[1], m.Y[-1], m.Z[1], m.Z[-1]]
    for dev in others:
        pl.semaphore_signal(barrier, inc=1, device_id=dev, device_id_type=MESH)
    pl.semaphore_wait(barrier, len(others))


def front_kernel(hid, wq, wk, wv, gain, cos, sin, q_out, kv_out, H, N, RH, W, acc, ssem, rsem, lsem):
    m = places()
    net = Net(ssem, rsem)
    c, t, d = m.c, m.t, m.d
    local = [
        pltpu.make_async_copy(wq, W.at[c, d, :, pl.ds(0, 512)], lsem.at[0]),
        pltpu.make_async_copy(wk, W.at[c, d, :, pl.ds(512, 128)], lsem.at[1]),
        pltpu.make_async_copy(wv, W.at[c, d, :, pl.ds(640, 128)], lsem.at[2]),
        pltpu.make_async_copy(hid.at[0], H.at[t], lsem.at[3]),
    ]
    for cp in local:
        cp.start()
    greet(m)
    for cp in local:
        cp.wait()

    def pair(z):
        return pl.ds(2 * z, 2)

    qa = {1: pl.ds(0, 32), -1: pl.ds(32, 32)}
    qb = {1: pl.ds(64, 32), -1: pl.ds(96, 32)}
    ha, hb = pl.ds(0, 64), pl.ds(64, 64)
    parts = 2
    rows = 256 // parts

    kX = net.send(W.at[c, d], m.P)
    kY1 = {s: net.send(W.at[c, d], m.Y[s]) for s in SIDES}
    kZ1 = {s: net.send(W.at[c, d], m.Z[s]) for s in SIDES}
    kH0 = [net.send(H.at[t, pl.ds(i * rows, rows)], m.P, RH.at[0, pl.ds(i * rows, rows)]) for i in range(parts)]
    kH1 = [net.send(H.at[t, pl.ds(256 + i * rows, rows)], m.Q, RH.at[1, pl.ds(i * rows, rows)]) for i in range(parts)]
    kC = net.send(H.at[t], m.C)

    net.recv(kX, W.at[m.c1, d])
    kY2 = {s: net.send(W.at[m.c1, d], m.Y[s]) for s in SIDES}
    kZ2 = {s: net.send(W.at[m.c1, d], m.Z[s]) for s in SIDES}

    fY, fZ, kY3, kZ3, kY4, kZ4 = {}, {}, {}, {}, {}, {}
    for s in SIDES:
        net.recv(kY1[s], W.at[c, m.yo[s]])
        net.recv(kZ1[s], W.at[2 * m.zo[s] + m.xl, d])
    for s in SIDES:
        net.recv(kY2[s], W.at[m.c1, m.yo[s]])
        kY3[s] = net.send(W.at[pair(m.z), m.yo[s], qa[s]], m.Y[s])
        net.recv(kZ2[s], W.at[2 * m.zo[s] + m.xo, d])
        kZ3[s] = net.send(W.at[pair(m.zo[s]), d, qb[s]], m.Z[s])
    for s in SIDES:
        for r in SIDES:
            kZ4[s, r] = net.send(W.at[pair(m.z), m.yo[s], ha], m.Z[r])
            kY4[s, r] = net.send(W.at[pair(m.zo[s]), d, hb], m.Y[r])

    def relay(i):
        net.recv(kH0[i], RH.at[0, pl.ds(i * rows, rows)])
        a = net.send(RH.at[0, pl.ds(i * rows, rows)], m.Q, H.at[t, pl.ds(i * rows, rows)])
        net.recv(kH1[i], RH.at[1, pl.ds(i * rows, rows)])
        b = net.send(RH.at[1, pl.ds(i * rows, rows)], m.P, H.at[m.t2, pl.ds(256 + i * rows, rows)])
        return a, b

    def landed(k):
        out = []
        for i in range(parts):
            for k_, lo in ((k[i][0], i * rows), (k[i][1], 256 + i * rows)):
                net.recv(k_, H.at[m.t2, pl.ds(lo, rows)])
                out.append((net.send(H.at[m.t2, pl.ds(lo, rows)], m.C), lo))
        return out

    kF = [relay(0)]
    kY6, kZ6 = {}, {}
    for s in SIDES:
        net.recv(kY3[s], W.at[pair(m.z), m.y2, qa[s]])
        net.recv(kZ3[s], W.at[pair(m.z2), d, qb[s]])
    for r in SIDES:
        kZ6[r] = net.send(W.at[pair(m.z), m.y2, ha], m.Z[r])
        kY6[r] = net.send(W.at[pair(m.z2), d, hb], m.Y[r])
    for s in SIDES:
        fZ[s, "own"] = net.send(W.at[pair(m.zo[s]), d, qa[s]], m.Z[s])
        fY[s, "own"] = net.send(W.at[pair(m.z), m.yo[s], qb[s]], m.Y[s])
    kF += [relay(i) for i in range(1, parts)]
    for s in SIDES:
        for r in SIDES:
            net.recv(kZ4[s, r], W.at[pair(m.zo[r]), m.yo[s], ha])
            fZ[r, s] = net.send(W.at[pair(m.zo[r]), m.yo[s], qa[r]], m.Z[r])
            net.recv(kY4[s, r], W.at[pair(m.zo[s]), m.yo[r], hb])
            fY[r, s] = net.send(W.at[pair(m.zo[s]), m.yo[r], qb[r]], m.Y[r])
    for r in SIDES:
        net.recv(kZ6[r], W.at[pair(m.zo[r]), m.y2, ha])
        fZ[r, "far"] = net.send(W.at[pair(m.zo[r]), m.y2, qa[r]], m.Z[r])
        net.recv(kY6[r], W.at[pair(m.z2), m.yo[r], hb])
        fY[r, "far"] = net.send(W.at[pair(m.z2), m.yo[r], qb[r]], m.Y[r])
    far = landed(kF)
    net.recv(kC, H.at[m.t1])
    for k, lo in far:
        net.recv(k, H.at[m.t3, pl.ds(lo, rows)])

    step = 64

    def norm(i, carry):
        at = pl.ds(pl.multiple_of(i * step, step), step)
        total = jnp.zeros((step, 1), jnp.float32)
        for b in range(4):
            x = H[b, at, :].astype(jnp.float32)
            total = total + jnp.sum(x * x, axis=1, keepdims=True)
        scale = lax.rsqrt(total * (1.0 / MODEL_WIDTH) + 1e-05)
        for b in range(4):
            x = H[b, at, :].astype(jnp.float32)
            g = gain[:, b * 1024 : (b + 1) * 1024]
            N[b, at, :] = (x * scale * g).astype(jnp.bfloat16)
        return carry

    lax.fori_loop(0, 512 // step, norm, 0)

    def chunk(z, first):
        for n in range(3):
            cols = pl.ds(n * 256, 256)
            w = W[pair(z), :, :, cols].reshape(1024, 256)
            part = jnp.dot(N[z], w, preferred_element_type=jnp.float32)
            if first:
                acc[:, cols] = part
            else:
                acc[:, cols] += part

    for r in SIDES:
        net.recv(fY[r, "own"], W.at[pair(m.z), m.y2, qb[r]])
    chunk(m.z, True)
    for s in SIDES:
        for r in SIDES:
            net.recv(fY[r, s], W.at[pair(m.zo[s]), m.y2, qb[r]])
    for s in SIDES:
        chunk(m.zo[s], False)
    for r in SIDES:
        net.recv(fZ[r, "own"], W.at[pair(m.z2), d, qa[r]])
        for s in SIDES:
            net.recv(fZ[r, s], W.at[pair(m.z2), m.yo[s], qa[r]])
        net.recv(fZ[r, "far"], W.at[pair(m.z2), m.y2, qa[r]])
        net.recv(fY[r, "far"], W.at[pair(m.z2), m.y2, qb[r]])
    chunk(m.z2, False)

    def rope(i, carry):
        at = pl.ds(pl.multiple_of(i * step, step), step)
        co, si = cos[at, :], sin[at, :]
        for h in range(5):
            x = acc[at, h * 128 : (h + 1) * 128]
            y = (x * co + pltpu.roll(x, 64, 1) * si).astype(jnp.bfloat16)
            if h < 4:
                q_out[h, at, :] = y
            else:
                kv_out[0, at, :] = y
        kv_out[1, at, :] = acc[at, 640:768].astype(jnp.bfloat16)
        return carry

    lax.fori_loop(0, 512 // step, rope, 0)
    net.finish()


def front(hidden, wq, wk, wv, gain, cos, sin):
    any_spec = pl.BlockSpec(memory_space=pl.ANY)
    vmem = pl.BlockSpec(memory_space=pltpu.VMEM)
    return pl.pallas_call(
        front_kernel,
        out_shape=(
            jax.ShapeDtypeStruct((4, 512, 128), jnp.bfloat16),
            jax.ShapeDtypeStruct((2, 512, 128), jnp.bfloat16),
        ),
        in_specs=[any_spec] * 4 + [vmem] * 3,
        out_specs=(vmem, vmem),
        scratch_shapes=[
            pltpu.VMEM((4, 512, 1024), jnp.bfloat16),
            pltpu.VMEM((4, 512, 1024), jnp.bfloat16),
            pltpu.VMEM((2, 256, 1024), jnp.bfloat16),
            pltpu.VMEM((8, 4, 128, 768), jnp.bfloat16),
            pltpu.VMEM((512, 768), jnp.float32),
            pltpu.SemaphoreType.DMA((64,)),
            pltpu.SemaphoreType.DMA((64,)),
            pltpu.SemaphoreType.DMA((4,)),
        ],
        compiler_params=pltpu.CompilerParams(
            collective_id=0, has_side_effects=True, vmem_limit_bytes=60 * 1024 * 1024
        ),
        name="front",
    )(hidden, wq, wk, wv, gain, cos, sin)


def attend(state, query_rows, qpos, piece, kpos):
    peak, total, accum = state
    rows = piece.shape[1]
    local_heads = query_rows.shape[1]
    pair = piece.reshape(2, rows, local_heads, HEAD_SIZE)
    scores = jnp.einsum(
        "qcgd,kcd->cgqk", query_rows, pair[0], preferred_element_type=jnp.float32
    ) * (1.0 / HEAD_SIZE**0.5)
    allowed = (qpos[:, None] >= kpos[None, :])[None, None]
    scores = jnp.where(allowed, scores, -1e30)
    new_peak = jnp.maximum(peak, jnp.max(scores, axis=-1))
    weights = jnp.where(allowed, jnp.exp(scores - new_peak[..., None]), 0.0)
    factor = jnp.exp(peak - new_peak)
    total = total * factor + jnp.sum(weights, axis=-1)
    update = jnp.einsum(
        "cgqk,kcd->qcgd", weights.astype(jnp.bfloat16), pair[1], preferred_element_type=jnp.float32
    )
    accum = accum * jnp.transpose(factor, (2, 0, 1))[..., None] + update
    return (new_peak, total, accum)


def on_device(hidden, target, gain, w_query, w_key, value_matrix, w_out, block_order):
    rows = hidden.shape[1]
    half = rows // 2
    local = hidden[0]
    shard = lax.axis_index(CTX)
    qpos = positions(block_order, shard * rows, rows, half)
    local_heads = w_key.shape[1] // HEAD_SIZE
    query_group = QUERY_HEADS // KEY_VALUE_HEADS
    angles = qpos.astype(jnp.float32)[:, None] * (rope_base ** (-(jnp.arange(64, dtype=jnp.float32) * 2.0) / 128))[None, :]
    co, si = jnp.cos(angles), jnp.sin(angles)
    co, si = jnp.concatenate([co, co], 1), jnp.concatenate([-si, si], 1)
    q, pair = front(hidden, w_query, w_key, value_matrix, gain[None, :], co, si)
    query_rows = jnp.transpose(q, (1, 0, 2)).reshape(rows, local_heads, query_group, HEAD_SIZE)
    state = (
        jnp.full((local_heads, query_group, rows), -1e30, jnp.float32),
        jnp.zeros((local_heads, query_group, rows), jnp.float32),
        jnp.zeros((rows, local_heads, query_group, HEAD_SIZE), jnp.float32),
    )
    count = lax.axis_size(CTX)
    state = attend(state, query_rows, qpos, pair, qpos)

    def turn(step, carry):
        moved, inner = carry
        moved = shifted(moved, CTX, 1)
        source = (shard - step) % count
        return (
            moved,
            attend(
                inner, query_rows, qpos, moved, positions(block_order, source * rows, rows, half)
            ),
        )

    moved_end, state = lax.fori_loop(1, count, turn, (pair, state))
    peak, total, accum = state
    attn = (
        (accum / jnp.transpose(total, (2, 0, 1))[..., None])
        .astype(jnp.bfloat16)
        .reshape(rows, local_heads * query_group * HEAD_SIZE)
    )
    terms = jnp.dot(
        attn, lax.all_gather(w_out, CTX_DP, axis=1, tiled=True), preferred_element_type=jnp.float32
    )
    summed = lax.psum_scatter(terms.astype(jnp.bfloat16), TP, scatter_dimension=1, tiled=True)
    resid = local.astype(jnp.float32) + summed.astype(jnp.float32) - target[0].astype(jnp.float32)
    squares = lax.psum(jnp.sum(resid * resid), CTX_TP_DP)
    loss = squares / (lax.axis_size("dp") * lax.axis_size(CTX) * rows * MODEL_WIDTH)
    return (summed[None], loss)


def solution(mesh):
    placed = (
        P("dp", CTX, TP),
        P("dp", CTX, TP),
        P(),
        P(CTX_DP, TP),
        P(CTX_DP, TP),
        P(CTX_DP, TP),
        P(TP, CTX_DP),
        P(),
    )
    return jax.shard_map(
        on_device, mesh=mesh, in_specs=placed, out_specs=(P("dp", CTX, TP), P()), check_vma=False
    )
```

```python
import types

import jax
import jax.numpy as jnp
import numpy as np
from jax import lax
from jax.experimental import pallas as pl
from jax.experimental.pallas import tpu as pltpu
from jax.sharding import PartitionSpec as P

MODEL_WIDTH = 4096
HEAD_SIZE = 128
ROPE_BASE = 500000.0
NEG = -1e30
SCALE = float(np.log2(np.e) / np.sqrt(HEAD_SIZE))
MIB = 1024 * 1024

MESH = pl.DeviceIdType.MESH
SIDES = (1, -1)


def here():
    c, t, d = lax.axis_index("ctx"), lax.axis_index("tp"), lax.axis_index("dp")
    return c, t, d


class Net:
    def __init__(self, send_sems, recv_sems):
        self.send_sems, self.recv_sems = send_sems, recv_sems
        self.started = []

    def copy(self, k, src, dst, dev):
        c, t, d = dev
        return pltpu.make_async_remote_copy(
            src_ref=src,
            dst_ref=dst,
            send_sem=self.send_sems.at[k],
            recv_sem=self.recv_sems.at[k],
            device_id=(c, t, d),
            device_id_type=MESH,
        )

    def send(self, ref, dev, dst=None):
        k = len(self.started)
        copy = self.copy(k, ref, ref if dst is None else dst, dev)
        copy.start()
        self.started.append((copy, dev))
        return k

    def recv(self, k, ref):
        self.copy(k, ref, ref, self.started[k][1]).wait_recv()

    def finish(self):
        for copy, _ in self.started:
            copy.wait_send()


def places():
    c, t, d = here()
    z, xl = c // 2, c % 2
    c1 = c + 1 - 2 * xl
    t1 = t + 1 - 2 * (t % 2)
    t2 = (t + 2) % 4
    t3 = (t1 + 2) % 4
    return types.SimpleNamespace(
        c=c, t=t, d=d, z=z, xl=xl, xo=1 - xl, c1=c1, t1=t1, t2=t2, t3=t3,
        P=(c1, t, d), Q=(c1, t2, d), C=(c, t1, d), R=(c, t2, d), D=(c, t3, d),
        Y={s: (c, t, (d + s) % 4) for s in SIDES},
        Z={s: ((c + 2 * s) % 8, t, d) for s in SIDES},
        yo={s: (d - s) % 4 for s in SIDES},
        zo={s: (z - s) % 4 for s in SIDES},
        y2=(d + 2) % 4, z2=(z + 2) % 4,
        far=((c1, t1, d), (c1, t3, d), (c, t, (d + 2) % 4), ((c + 4) % 8, t, d)),
    )


def greet(m):
    barrier = pltpu.get_barrier_semaphore()
    others = [m.P, m.Q, m.C, m.R, m.D, m.Y[1], m.Y[-1], m.Z[1], m.Z[-1], *m.far]
    for dev in others:
        pl.semaphore_signal(barrier, inc=1, device_id=dev, device_id_type=MESH)
    pl.semaphore_wait(barrier, len(others))


def layer_kernel(
    hid, tgt, wq, wk, wv, wo, gain, order, row_cos, row_sin, block_cos, block_sin,
    out, loss_out,
    H, N, RH, W, acc, Q, KV, WO, AT, RA, num, peak, T, total, LB, ssem, rsem, lsem, osend, orecv,
):
    m = places()
    net = Net(ssem, rsem)
    c, t, d = m.c, m.t, m.d
    local = [
        pltpu.make_async_copy(wq, W.at[c, d, :, pl.ds(0, 512)], lsem.at[0]),
        pltpu.make_async_copy(wk, W.at[c, d, :, pl.ds(512, 128)], lsem.at[1]),
        pltpu.make_async_copy(wv, W.at[c, d, :, pl.ds(640, 128)], lsem.at[2]),
        pltpu.make_async_copy(hid.at[0], H.at[t], lsem.at[3]),
    ]
    for cp in local:
        cp.start()
    later = pltpu.make_async_copy(tgt.at[0], T, lsem.at[4])
    later.start()
    own_wo = pltpu.make_async_copy(wo, WO.at[m.xl * 4 + d, pl.ds(m.z * 512, 512)], lsem.at[5])
    greet(m)
    for cp in local:
        cp.wait()

    def pair(z):
        return pl.ds(2 * z, 2)

    qa = {1: pl.ds(0, 32), -1: pl.ds(32, 32)}
    qb = {1: pl.ds(64, 32), -1: pl.ds(96, 32)}
    ha, hb = pl.ds(0, 64), pl.ds(64, 64)
    parts = 2
    rows = 256 // parts

    kX = net.send(W.at[c, d], m.P)
    kY1 = {s: net.send(W.at[c, d], m.Y[s]) for s in SIDES}
    kZ1 = {s: net.send(W.at[c, d], m.Z[s]) for s in SIDES}
    kH0 = [net.send(H.at[t, pl.ds(i * rows, rows)], m.P, RH.at[0, pl.ds(i * rows, rows)]) for i in range(parts)]
    kH1 = [net.send(H.at[t, pl.ds(256 + i * rows, rows)], m.Q, RH.at[1, pl.ds(i * rows, rows)]) for i in range(parts)]
    kC = net.send(H.at[t], m.C)

    mine = WO.at[m.xl * 4 + d]
    block = WO.at[m.xl * 4 + d, pl.ds(t * 512, 512)]

    def meet(k):
        return pltpu.make_async_remote_copy(
            src_ref=wo, dst_ref=block, send_sem=osend.at[4], recv_sem=orecv.at[4 + k],
            device_id=(c, m.z, d), device_id_type=MESH,
        )

    @pl.when(t == m.z)
    def _():
        own_wo.start()

    @pl.when(t != m.z)
    def _():
        meet(t).start()

    net.recv(kX, W.at[m.c1, d])
    kY2 = {s: net.send(W.at[m.c1, d], m.Y[s]) for s in SIDES}
    kZ2 = {s: net.send(W.at[m.c1, d], m.Z[s]) for s in SIDES}

    fY, fZ, kY3, kZ3, kY4, kZ4 = {}, {}, {}, {}, {}, {}
    for s in SIDES:
        net.recv(kY1[s], W.at[c, m.yo[s]])
        net.recv(kZ1[s], W.at[2 * m.zo[s] + m.xl, d])
    for s in SIDES:
        net.recv(kY2[s], W.at[m.c1, m.yo[s]])
        kY3[s] = net.send(W.at[pair(m.z), m.yo[s], qa[s]], m.Y[s])
        net.recv(kZ2[s], W.at[2 * m.zo[s] + m.xo, d])
        kZ3[s] = net.send(W.at[pair(m.zo[s]), d, qb[s]], m.Z[s])
    for s in SIDES:
        for r in SIDES:
            kZ4[s, r] = net.send(W.at[pair(m.z), m.yo[s], ha], m.Z[r])
            kY4[s, r] = net.send(W.at[pair(m.zo[s]), d, hb], m.Y[r])

    def relay(i):
        net.recv(kH0[i], RH.at[0, pl.ds(i * rows, rows)])
        a = net.send(RH.at[0, pl.ds(i * rows, rows)], m.Q, H.at[t, pl.ds(i * rows, rows)])
        net.recv(kH1[i], RH.at[1, pl.ds(i * rows, rows)])
        b = net.send(RH.at[1, pl.ds(i * rows, rows)], m.P, H.at[m.t2, pl.ds(256 + i * rows, rows)])
        return a, b

    def landed(k):
        out = []
        for i in range(parts):
            for k_, lo in ((k[i][0], i * rows), (k[i][1], 256 + i * rows)):
                net.recv(k_, H.at[m.t2, pl.ds(lo, rows)])
                out.append((net.send(H.at[m.t2, pl.ds(lo, rows)], m.C), lo))
        return out

    kF = [relay(0)]
    kY6, kZ6 = {}, {}
    for s in SIDES:
        net.recv(kY3[s], W.at[pair(m.z), m.y2, qa[s]])
        net.recv(kZ3[s], W.at[pair(m.z2), d, qb[s]])
    for r in SIDES:
        kZ6[r] = net.send(W.at[pair(m.z), m.y2, ha], m.Z[r])
        kY6[r] = net.send(W.at[pair(m.z2), d, hb], m.Y[r])
    for s in SIDES:
        fZ[s, "own"] = net.send(W.at[pair(m.zo[s]), d, qa[s]], m.Z[s])
        fY[s, "own"] = net.send(W.at[pair(m.z), m.yo[s], qb[s]], m.Y[s])
    kF += [relay(i) for i in range(1, parts)]
    for s in SIDES:
        for r in SIDES:
            net.recv(kZ4[s, r], W.at[pair(m.zo[r]), m.yo[s], ha])
            fZ[r, s] = net.send(W.at[pair(m.zo[r]), m.yo[s], qa[r]], m.Z[r])
            net.recv(kY4[s, r], W.at[pair(m.zo[s]), m.yo[r], hb])
            fY[r, s] = net.send(W.at[pair(m.zo[s]), m.yo[r], qb[r]], m.Y[r])
    for r in SIDES:
        net.recv(kZ6[r], W.at[pair(m.zo[r]), m.y2, ha])
        fZ[r, "far"] = net.send(W.at[pair(m.zo[r]), m.y2, qa[r]], m.Z[r])
        net.recv(kY6[r], W.at[pair(m.z2), m.yo[r], hb])
        fY[r, "far"] = net.send(W.at[pair(m.z2), m.yo[r], qb[r]], m.Y[r])
    far = landed(kF)
    net.recv(kC, H.at[m.t1])
    for k, lo in far:
        net.recv(k, H.at[m.t3, pl.ds(lo, rows)])


    turn = (m.z - t + 4) % 4

    def along(k, ref, s):
        return pltpu.make_async_remote_copy(
            src_ref=ref, dst_ref=ref, send_sem=osend.at[k], recv_sem=orecv.at[k],
            device_id=m.Z[s], device_id_type=MESH,
        )

    low = WO.at[m.xl * 4 + d, pl.ds(0, 1024)]
    high = WO.at[m.xl * 4 + d, pl.ds(1024, 1024)]

    @pl.when(turn == 0)
    def _():
        own_wo.wait()
        for k in range(4):
            @pl.when(k != t)
            def _(k=k):
                there = WO.at[m.xl * 4 + d, pl.ds(k * 512, 512)]
                pltpu.make_async_remote_copy(
                    src_ref=there, dst_ref=there, send_sem=osend.at[4], recv_sem=orecv.at[4 + k],
                    device_id=(c, m.z, d), device_id_type=MESH,
                ).wait_recv()

        along(0, mine, 1).start()
        along(1, mine, -1).start()

    step = 64

    def norm(i, carry):
        at = pl.ds(pl.multiple_of(i * step, step), step)
        total = jnp.zeros((step, 1), jnp.float32)
        for b in range(4):
            x = H[b, at, :].astype(jnp.float32)
            total = total + jnp.sum(x * x, axis=1, keepdims=True)
        scale = lax.rsqrt(total * (1.0 / MODEL_WIDTH) + 1e-05)
        for b in range(4):
            x = H[b, at, :].astype(jnp.float32)
            g = gain[:, b * 1024 : (b + 1) * 1024]
            N[b, at, :] = (x * scale * g).astype(jnp.bfloat16)
        return carry

    lax.fori_loop(0, 512 // step, norm, 0)

    def chunk(z, first):
        for n in range(3):
            cols = pl.ds(n * 256, 256)
            w = W[pair(z), :, :, cols].reshape(1024, 256)
            part = jnp.dot(N[z], w, preferred_element_type=jnp.float32)
            if first:
                acc[:, cols] = part
            else:
                acc[:, cols] += part

    for r in SIDES:
        net.recv(fY[r, "own"], W.at[pair(m.z), m.y2, qb[r]])
    chunk(m.z, True)
    for s in SIDES:
        for r in SIDES:
            net.recv(fY[r, s], W.at[pair(m.zo[s]), m.y2, qb[r]])
    for s in SIDES:
        chunk(m.zo[s], False)
    for r in SIDES:
        net.recv(fZ[r, "own"], W.at[pair(m.z2), d, qa[r]])
        for s in SIDES:
            net.recv(fZ[r, s], W.at[pair(m.z2), m.yo[s], qa[r]])
        net.recv(fZ[r, "far"], W.at[pair(m.z2), m.y2, qa[r]])
        net.recv(fY[r, "far"], W.at[pair(m.z2), m.y2, qb[r]])
    chunk(m.z2, False)

    for s in range(2):
        where = order[2 * c + s]
        bc, bs = block_cos[pl.ds(where, 1), :], block_sin[pl.ds(where, 1), :]

        def rope(i, carry, s=s, bc=bc, bs=bs):
            rows_at = pl.ds(pl.multiple_of(i * step, step), step)
            at = pl.ds(pl.multiple_of(s * 256 + i * step, step), step)
            rc, rs = row_cos[rows_at, :], row_sin[rows_at, :]
            co = rc * bc - rs * bs
            si = rs * bc + rc * bs
            lane = lax.broadcasted_iota(jnp.int32, (step, 128), 1)
            si = jnp.where(lane < 64, -si, si)
            for h in range(5):
                x = acc[at, h * 128 : (h + 1) * 128]
                y = (x * co + pltpu.roll(x, 64, 1) * si).astype(jnp.bfloat16)
                if h < 4:
                    Q[h, at, :] = y
                else:
                    KV[c, 0, at, :] = y
            KV[c, 1, at, :] = acc[at, 640:768].astype(jnp.bfloat16)
            return carry

        lax.fori_loop(0, 256 // step, rope, 0)

    kv0 = net.send(KV.at[c], m.P)
    kv1 = {s: net.send(KV.at[c], m.Z[s]) for s in SIDES}

    @pl.when(turn == 1)
    def _():
        along(0, mine, 1).wait_recv()
        along(2, low, 1).start()

    @pl.when(turn == 3)
    def _():
        along(1, mine, -1).wait_recv()
        along(3, high, -1).start()

    def bias(s, ctx, half):
        return jnp.where(order[2 * ctx + half] < order[2 * c + s], 0.0, NEG).astype(jnp.float32)

    ones = jnp.ones((512, 128), jnp.bfloat16)
    row = lax.broadcasted_iota(jnp.int32, (256, 256), 0)
    col = lax.broadcasted_iota(jnp.int32, (256, 256), 1)

    def tile(h, s, ctx, first, lift):
        at = pl.ds(s * 256, 256)
        q = Q[h, at, :]
        scores = lax.dot_general(q, KV[ctx, 0], (((1,), (1,)), ((), ())), preferred_element_type=jnp.float32)
        halves = [scores[:, :256], scores[:, 256:]]
        if first:
            halves[s] = jnp.where(row >= col, halves[s], NEG)
        tops = [jnp.max(x, axis=1, keepdims=True) * SCALE + b for x, b in zip(halves, lift)]
        new = jnp.maximum(tops[0], tops[1])
        if not first:
            old = peak[h, at, :1]
            new = jnp.maximum(old, new)
        p = [jnp.exp2(x * SCALE + (b - new)).astype(jnp.bfloat16) for x, b in zip(halves, lift)]
        value = jnp.concatenate([KV[ctx, 1], ones], axis=1)
        part = jnp.dot(jnp.concatenate(p, axis=1), value, preferred_element_type=jnp.float32)
        if not first:
            part = num[h, at, :] * jnp.exp2(old - new) + part
        peak[h, at, :] = jnp.broadcast_to(new, (256, 128))
        num[h, at, :] = part

    def lifts(ctx, first):
        out = {}
        for s in range(2):
            out[s] = [bias(s, ctx, half) for half in range(2)]
            if first:
                out[s][s] = jnp.float32(0.0)
        return out

    def attend(ctx, first=False):
        lift = lifts(ctx, first)

        def head(h, carry):
            for s in range(2):
                tile(h, s, ctx, first, lift[s])
            return carry

        lax.fori_loop(0, 4, head, 0)

    attend(c, True)
    net.recv(kv0, KV.at[m.c1])
    kv2 = {s: net.send(KV.at[m.c1], m.Z[s]) for s in SIDES}

    @pl.when(turn == 2)
    def _():
        along(2, low, 1).wait_recv()
        along(3, high, -1).wait_recv()

    def strip(xl, y, s=None):
        return WO.at[xl * 4 + y] if s is None else WO.at[xl * 4 + y, pl.ds(0 if s == 1 else 1024, 1024)]

    wo0 = net.send(mine, m.P)
    wo1 = {s: net.send(mine, m.Y[s]) for s in SIDES}
    kv3, kv4, wo2, wo3, wo4 = {}, {}, {}, {}, {}
    part_of = {1: 0, -1: 1}
    for s in SIDES:
        there = 2 * m.zo[s] + m.xl
        net.recv(kv1[s], KV.at[there])
        kv3[s] = net.send(KV.at[there, part_of[s]], m.Z[s])
    for s in SIDES:
        attend(2 * m.zo[s] + m.xl)
    attend(m.c1)
    net.recv(wo0, strip(m.xo, d))
    for s in SIDES:
        wo2[s] = net.send(strip(m.xo, d), m.Y[s])
    for s in SIDES:
        there = 2 * m.zo[s] + m.xo
        net.recv(kv2[s], KV.at[there])
        kv4[s] = net.send(KV.at[there, part_of[s]], m.Z[s])
    for s in SIDES:
        attend(2 * m.zo[s] + m.xo)
    for s in SIDES:
        net.recv(wo1[s], strip(m.xl, m.yo[s]))
        wo3[s] = net.send(strip(m.xl, m.yo[s], s), m.Y[s])
    for s in SIDES:
        net.recv(kv3[s], KV.at[2 * m.z2 + m.xl, part_of[s]])
    for s in SIDES:
        net.recv(kv4[s], KV.at[2 * m.z2 + m.xo, part_of[s]])

    last = [(ctx, lifts(ctx, False)) for ctx in (2 * m.z2 + m.xl, 2 * m.z2 + m.xo)]
    top, bottom = pl.ds(0, 256), pl.ds(256, 256)
    kA = []
    for h in range(4):
        for ctx, lift in last:
            for s in range(2):
                tile(h, s, ctx, False, lift[s])
        both = num[h]
        AT[t, h] = (both[:, :128] / both[:, 128:]).astype(jnp.bfloat16)
        kA.append((
            net.send(AT.at[t, h, top], m.P, RA.at[0, h]),
            net.send(AT.at[t, h, bottom], m.Q, RA.at[1, h]),
            net.send(AT.at[t, h], m.C),
        ))
    for s in SIDES:
        net.recv(wo2[s], strip(m.xo, m.yo[s]))
        wo4[s] = net.send(strip(m.xo, m.yo[s], s), m.Y[s])
    kR = []
    for h in range(4):
        net.recv(kA[h][0], RA.at[0, h])
        a = net.send(RA.at[0, h], m.Q, AT.at[t, h, top])
        net.recv(kA[h][1], RA.at[1, h])
        kR.append((a, net.send(RA.at[1, h], m.P, AT.at[m.t2, h, bottom])))
    kD = []
    for h in range(4):
        net.recv(kR[h][0], AT.at[m.t2, h, top])
        net.recv(kR[h][1], AT.at[m.t2, h, bottom])
        kD.append(net.send(AT.at[m.t2, h], m.C))

    for s in SIDES:
        net.recv(wo3[s], strip(m.xl, m.y2, s))
        net.recv(wo4[s], strip(m.xo, m.y2, s))

    def project(b, first):
        left = jnp.concatenate([AT[b, h] for h in range(4)], axis=1)
        for j in range(4):
            right = jnp.concatenate([WO[2 * j + i, pl.ds(b * 512, 512), :] for i in range(2)], axis=1)
            part = jnp.dot(left, right, preferred_element_type=jnp.float32)
            cols = pl.ds(j * 256, 256)
            if first:
                total[:, cols] = part
            else:
                total[:, cols] += part

    project(t, True)
    for h in range(4):
        net.recv(kA[h][2], AT.at[m.t1, h])
    project(m.t1, False)
    project(m.t2, False)
    for h in range(4):
        net.recv(kD[h], AT.at[m.t3, h])
    project(m.t3, False)
    later.wait()

    def close(i, carry):
        at = pl.ds(pl.multiple_of(i * 32, 32), 32)
        branch = total[at, :].astype(jnp.bfloat16)
        out[0, at, :] = branch
        gap = H[t, at, :].astype(jnp.float32) + branch.astype(jnp.float32) - T[at, :].astype(jnp.float32)
        sq = gap * gap
        for r in range(4):
            for b in range(8):
                carry = carry + sq[r * 8 : (r + 1) * 8, b * 128 : (b + 1) * 128]
        return carry

    part = lax.fori_loop(0, 16, close, jnp.zeros((8, 128), jnp.float32))
    rings = (
        (8, m.xl * 4 + t, lambda i: (2 * m.z + i // 4, i % 4, d)),
        (4, d, lambda i: (c, t, i)),
        (4, m.z, lambda i: (2 * i + m.xl, t, d)),
    )
    for number, (size, me, device) in enumerate(rings):
        LB[number, me] = part
        ks = [net.send(LB.at[number, me], device((me + j) % size)) for j in range(1, size)]
        for j in range(1, size):
            net.recv(ks[j - 1], LB.at[number, (me + size - j) % size])
        part = LB[number, 0]
        for j in range(1, size):
            part = part + LB[number, j]
    loss_out[0, 0] = jnp.sum(part) / (4 * 4096 * MODEL_WIDTH)
    net.finish()

    @pl.when(t != m.z)
    def _():
        meet(t).wait_send()

    for k, ref, s, when in ((0, mine, 1, 0), (1, mine, -1, 0), (2, low, 1, 1), (3, high, -1, 3)):
        @pl.when(turn == when)
        def _(k=k, ref=ref, s=s):
            along(k, ref, s).wait_send()


def tables():
    freqs = ROPE_BASE ** (-(np.arange(64) * 2.0) / HEAD_SIZE)
    freqs = np.concatenate([freqs, freqs])[None, :]
    rows, blocks = np.arange(256)[:, None] * freqs, np.arange(16)[:, None] * 256 * freqs
    return [f(x).astype(np.float32) for x in (rows, blocks) for f in (np.cos, np.sin)]


def on_device(hidden, target, gain, w_query, w_key, value_matrix, w_out, block_order):
    any_spec = pl.BlockSpec(memory_space=pl.ANY)
    vmem = pl.BlockSpec(memory_space=pltpu.VMEM)
    smem = pl.BlockSpec(memory_space=pltpu.SMEM)
    bf16, f32 = jnp.bfloat16, jnp.float32
    branch, loss = pl.pallas_call(
        layer_kernel,
        out_shape=(jax.ShapeDtypeStruct((1, 512, 1024), bf16), jax.ShapeDtypeStruct((1, 1), f32)),
        in_specs=[any_spec] * 6 + [vmem, smem] + [vmem] * 4,
        out_specs=(vmem, smem),
        scratch_shapes=[
            pltpu.VMEM((4, 512, 1024), bf16),
            pltpu.VMEM((4, 512, 1024), bf16),
            pltpu.VMEM((2, 256, 1024), bf16),
            pltpu.VMEM((8, 4, 128, 768), bf16),
            pltpu.VMEM((512, 768), f32),
            pltpu.VMEM((4, 512, 128), bf16),
            pltpu.VMEM((8, 2, 512, 128), bf16),
            pltpu.VMEM((8, 2048, 128), bf16),
            pltpu.VMEM((4, 4, 512, 128), bf16),
            pltpu.VMEM((2, 4, 256, 128), bf16),
            pltpu.VMEM((4, 512, 256), f32),
            pltpu.VMEM((4, 512, 128), f32),
            pltpu.VMEM((512, 1024), bf16),
            pltpu.VMEM((512, 1024), f32),
            pltpu.VMEM((3, 8, 8, 128), f32),
            pltpu.SemaphoreType.DMA((128,)),
            pltpu.SemaphoreType.DMA((128,)),
            pltpu.SemaphoreType.DMA((8,)),
            pltpu.SemaphoreType.DMA((8,)),
            pltpu.SemaphoreType.DMA((8,)),
        ],
        compiler_params=pltpu.CompilerParams(
            collective_id=0, has_side_effects=True, vmem_limit_bytes=60 * MIB
        ),
        name="layer",
    )(hidden, target, w_query, w_key, value_matrix, w_out, gain[None, :], block_order, *(jnp.asarray(x) for x in tables()))
    return branch, loss.reshape(())


def solution(mesh):
    placed = (
        P("dp", "ctx", "tp"), P("dp", "ctx", "tp"), P(), P(("ctx", "dp"), "tp"), P(("ctx", "dp"), "tp"),
        P(("ctx", "dp"), "tp"), P("tp", ("ctx", "dp")), P(),
    )
    return jax.shard_map(
        on_device, mesh=mesh, in_specs=placed, out_specs=(P("dp", "ctx", "tp"), P()), check_vma=False
    )
```

```python
import types

import jax
import jax.numpy as jnp
import numpy as np
from jax import lax
from jax.experimental import pallas as pl
from jax.experimental.pallas import tpu as pltpu
from jax.sharding import PartitionSpec as P

MODEL_WIDTH = 4096
HEAD_SIZE = 128
ROPE_BASE = 500000.0
NEG = -1e30
SCALE = float(np.log2(np.e) / np.sqrt(HEAD_SIZE))
MIB = 1024 * 1024
POOL = 40
COPIES = 120

MESH = pl.DeviceIdType.MESH
SIDES = (1, -1)


def here():
    c, t, d = lax.axis_index("ctx"), lax.axis_index("tp"), lax.axis_index("dp")
    return c, t, d


class Net:
    def __init__(self, send_sems, recv_sems):
        self.send_sems, self.recv_sems = send_sems, recv_sems
        self.started = []

    def copy(self, k, src, dst, dev):
        c, t, d = dev
        return pltpu.make_async_remote_copy(
            src_ref=src,
            dst_ref=dst,
            send_sem=self.send_sems.at[k % POOL],
            recv_sem=self.recv_sems.at[k],
            device_id=(c, t, d),
            device_id_type=MESH,
        )

    def plan(self, ref, dev, dst=None):
        k = len(self.started)
        if k >= POOL:
            self.started[k - POOL][0].wait_send()
        self.started.append((self.copy(k, ref, ref if dst is None else dst, dev), dev))
        return k

    def start(self, k):
        self.started[k][0].start()

    def send(self, ref, dev, dst=None):
        k = self.plan(ref, dev, dst)
        self.start(k)
        return k

    def recv(self, k, ref):
        self.copy(k, ref, ref, self.started[k][1]).wait_recv()

    def finish(self):
        assert len(self.started) <= COPIES
        for copy, _ in self.started[-POOL:]:
            copy.wait_send()


def places():
    c, t, d = here()
    z, xl = c // 2, c % 2
    c1 = c + 1 - 2 * xl
    t1 = t + 1 - 2 * (t % 2)
    t2 = (t + 2) % 4
    t3 = (t1 + 2) % 4
    return types.SimpleNamespace(
        c=c, t=t, d=d, z=z, xl=xl, xo=1 - xl, c1=c1, t1=t1, t2=t2, t3=t3,
        P=(c1, t, d), Q=(c1, t2, d), C=(c, t1, d), R=(c, t2, d), D=(c, t3, d),
        Y={s: (c, t, (d + s) % 4) for s in SIDES},
        Z={s: ((c + 2 * s) % 8, t, d) for s in SIDES},
        yo={s: (d - s) % 4 for s in SIDES},
        zo={s: (z - s) % 4 for s in SIDES},
        y2=(d + 2) % 4, z2=(z + 2) % 4,
    )


def greet(m):
    barrier = pltpu.get_barrier_semaphore()
    others = [m.P, m.Q, m.C, m.R, m.D, m.Y[1], m.Y[-1], m.Z[1], m.Z[-1]]
    for dev in others:
        pl.semaphore_signal(barrier, inc=1, device_id=dev, device_id_type=MESH)
    pl.semaphore_wait(barrier, len(others))


def layer_kernel(
    hid, tgt, wq, wk, wv, wo, gain, order, turn_cos, turn_sin, block_cos, block_sin,
    out, loss_out,
    H, N, RH, W, acc, Q, KV, WO, AT, RA, num, peak, T, total, LB, row_cos, row_sin, ssem, rsem, lsem, osend, orecv,
):
    m = places()
    net = Net(ssem, rsem)
    c, t, d = m.c, m.t, m.d
    local = [
        pltpu.make_async_copy(wq, W.at[c, d, :, pl.ds(0, 512)], lsem.at[0]),
        pltpu.make_async_copy(wk, W.at[c, d, :, pl.ds(512, 128)], lsem.at[1]),
        pltpu.make_async_copy(wv, W.at[c, d, :, pl.ds(640, 128)], lsem.at[2]),
        pltpu.make_async_copy(hid.at[0], H.at[t], lsem.at[3]),
    ]
    for cp in local:
        cp.start()
    later = pltpu.make_async_copy(tgt.at[0], T, lsem.at[4])
    later.start()
    turns = [
        pltpu.make_async_copy(turn_cos, row_cos, lsem.at[6]),
        pltpu.make_async_copy(turn_sin, row_sin, lsem.at[7]),
    ]
    for cp in turns:
        cp.start()
    own_wo = pltpu.make_async_copy(wo, WO.at[m.xl * 4 + d, pl.ds(m.z * 512, 512)], lsem.at[5])
    greet(m)
    for cp in local:
        cp.wait()

    def pair(z):
        return pl.ds(2 * z, 2)

    qa = {1: pl.ds(0, 32), -1: pl.ds(32, 32)}
    qb = {1: pl.ds(64, 32), -1: pl.ds(96, 32)}
    ha, hb = pl.ds(0, 64), pl.ds(64, 64)
    parts = 4
    rows = 256 // parts

    kX = net.send(W.at[c, d], m.P)
    kY1 = {s: net.send(W.at[c, d], m.Y[s]) for s in SIDES}
    kZ1 = {s: net.send(W.at[c, d], m.Z[s]) for s in SIDES}
    kH0 = [net.send(H.at[t, pl.ds(i * rows, rows)], m.P, RH.at[0, pl.ds(i * rows, rows)]) for i in range(parts)]
    kH1 = [net.send(H.at[t, pl.ds(256 + i * rows, rows)], m.Q, RH.at[1, pl.ds(i * rows, rows)]) for i in range(parts)]
    kC = net.send(H.at[t], m.C)

    mine = WO.at[m.xl * 4 + d]
    block = WO.at[m.xl * 4 + d, pl.ds(t * 512, 512)]

    def meet(k):
        return pltpu.make_async_remote_copy(
            src_ref=wo, dst_ref=block, send_sem=osend.at[4], recv_sem=orecv.at[4 + k],
            device_id=(c, m.z, d), device_id_type=MESH,
        )

    @pl.when(t == m.z)
    def _():
        own_wo.start()

    @pl.when(t != m.z)
    def _():
        meet(t).start()

    net.recv(kX, W.at[m.c1, d])
    kY2 = {s: net.send(W.at[m.c1, d], m.Y[s]) for s in SIDES}
    kZ2 = {s: net.send(W.at[m.c1, d], m.Z[s]) for s in SIDES}

    def relay(i):
        net.recv(kH0[i], RH.at[0, pl.ds(i * rows, rows)])
        a = net.send(RH.at[0, pl.ds(i * rows, rows)], m.Q, H.at[t, pl.ds(i * rows, rows)])
        net.recv(kH1[i], RH.at[1, pl.ds(i * rows, rows)])
        b = net.send(RH.at[1, pl.ds(i * rows, rows)], m.P, H.at[m.t2, pl.ds(256 + i * rows, rows)])
        return a, b

    far = []

    def landed(i):
        for k_, lo in ((kF[i][0], i * rows), (kF[i][1], 256 + i * rows)):
            net.recv(k_, H.at[m.t2, pl.ds(lo, rows)])
            far.append((net.send(H.at[m.t2, pl.ds(lo, rows)], m.C), lo))

    kF = []
    fY, fZ, kY3, kZ3, kY4, kZ4 = {}, {}, {}, {}, {}, {}
    for s in SIDES:
        net.recv(kY1[s], W.at[c, m.yo[s]])
        net.recv(kZ1[s], W.at[2 * m.zo[s] + m.xl, d])
    kF.append(relay(0))
    for s in SIDES:
        net.recv(kY2[s], W.at[m.c1, m.yo[s]])
        kY3[s] = net.send(W.at[pair(m.z), m.yo[s], qa[s]], m.Y[s])
        net.recv(kZ2[s], W.at[2 * m.zo[s] + m.xo, d])
        kZ3[s] = net.send(W.at[pair(m.zo[s]), d, qb[s]], m.Z[s])
    for s in SIDES:
        for r in SIDES:
            kZ4[s, r] = net.send(W.at[pair(m.z), m.yo[s], ha], m.Z[r])
            kY4[s, r] = net.send(W.at[pair(m.zo[s]), d, hb], m.Y[r])

    kF += [relay(1), relay(2)]
    kY6, kZ6 = {}, {}
    for s in SIDES:
        net.recv(kY3[s], W.at[pair(m.z), m.y2, qa[s]])
        net.recv(kZ3[s], W.at[pair(m.z2), d, qb[s]])
    for r in SIDES:
        kZ6[r] = net.send(W.at[pair(m.z), m.y2, ha], m.Z[r])
        kY6[r] = net.send(W.at[pair(m.z2), d, hb], m.Y[r])
    for s in SIDES:
        fZ[s, "own"] = net.send(W.at[pair(m.zo[s]), d, qa[s]], m.Z[s])
        fY[s, "own"] = net.send(W.at[pair(m.z), m.yo[s], qb[s]], m.Y[s])
    kF.append(relay(3))
    for s in SIDES:
        for r in SIDES:
            net.recv(kZ4[s, r], W.at[pair(m.zo[r]), m.yo[s], ha])
            fZ[r, s] = net.send(W.at[pair(m.zo[r]), m.yo[s], qa[r]], m.Z[r])
            net.recv(kY4[s, r], W.at[pair(m.zo[s]), m.yo[r], hb])
            fY[r, s] = net.send(W.at[pair(m.zo[s]), m.yo[r], qb[r]], m.Y[r])
    landed(0)
    landed(1)
    landed(2)
    landed(3)
    for r in SIDES:
        net.recv(kZ6[r], W.at[pair(m.zo[r]), m.y2, ha])
        fZ[r, "far"] = net.send(W.at[pair(m.zo[r]), m.y2, qa[r]], m.Z[r])
        net.recv(kY6[r], W.at[pair(m.z2), m.yo[r], hb])
        fY[r, "far"] = net.send(W.at[pair(m.z2), m.yo[r], qb[r]], m.Y[r])
    turn = (m.z - t + 4) % 4

    def along(k, ref, s):
        return pltpu.make_async_remote_copy(
            src_ref=ref, dst_ref=ref, send_sem=osend.at[k], recv_sem=orecv.at[k],
            device_id=m.Z[s], device_id_type=MESH,
        )

    low = WO.at[m.xl * 4 + d, pl.ds(0, 1024)]
    high = WO.at[m.xl * 4 + d, pl.ds(1024, 1024)]

    @pl.when(turn == 0)
    def _():
        own_wo.wait()
        for k in range(4):
            @pl.when(k != t)
            def _(k=k):
                there = WO.at[m.xl * 4 + d, pl.ds(k * 512, 512)]
                pltpu.make_async_remote_copy(
                    src_ref=there, dst_ref=there, send_sem=osend.at[4], recv_sem=orecv.at[4 + k],
                    device_id=(c, m.z, d), device_id_type=MESH,
                ).wait_recv()

        along(0, mine, 1).start()
        along(1, mine, -1).start()

    def strip(xl, y, s=None):
        return WO.at[xl * 4 + y] if s is None else WO.at[xl * 4 + y, pl.ds(0 if s == 1 else 1024, 1024)]

    wo1 = {s: net.plan(mine, m.Y[s]) for s in SIDES}

    @pl.when(turn == 0)
    def _():
        for s in SIDES:
            net.start(wo1[s])

    net.recv(kC, H.at[m.t1])
    for k, lo in far:
        net.recv(k, H.at[m.t3, pl.ds(lo, rows)])


    step = 64

    def norm(i, carry):
        at = pl.ds(pl.multiple_of(i * step, step), step)
        total = jnp.zeros((step, 1), jnp.float32)
        for b in range(4):
            x = H[b, at, :].astype(jnp.float32)
            total = total + jnp.sum(x * x, axis=1, keepdims=True)
        scale = lax.rsqrt(total * (1.0 / MODEL_WIDTH) + 1e-05)
        for b in range(4):
            x = H[b, at, :].astype(jnp.float32)
            g = gain[:, b * 1024 : (b + 1) * 1024]
            N[b, at, :] = (x * scale * g).astype(jnp.bfloat16)
        return carry

    lax.fori_loop(0, 512 // step, norm, 0)

    def columns(zs, lo):
        cols = pl.ds(lo, 256)
        sums = None
        for z in zs:
            w = W[pair(z), :, :, cols].reshape(1024, 256)
            part = jnp.dot(N[z], w, preferred_element_type=jnp.float32)
            sums = part if sums is None else sums + part
        return sums

    for r in SIDES:
        net.recv(fY[r, "own"], W.at[pair(m.z), m.y2, qb[r]])
        for s in SIDES:
            net.recv(fY[r, s], W.at[pair(m.zo[s]), m.y2, qb[r]])
    acc[:, pl.ds(512, 256)] = columns((m.z, m.zo[1], m.zo[-1]), 512)

    for r in SIDES:
        net.recv(fZ[r, "own"], W.at[pair(m.z2), d, qa[r]])
        for s in SIDES:
            net.recv(fZ[r, s], W.at[pair(m.z2), m.yo[s], qa[r]])
        net.recv(fZ[r, "far"], W.at[pair(m.z2), m.y2, qa[r]])
        net.recv(fY[r, "far"], W.at[pair(m.z2), m.y2, qb[r]])
    acc[:, pl.ds(512, 256)] += columns((m.z2,), 512)
    for cp in turns:
        cp.wait()

    def rotate(heads):
        for s in range(2):
            where = order[2 * c + s]
            bc, bs = block_cos[pl.ds(where, 1), :], block_sin[pl.ds(where, 1), :]

            def rope(i, carry, s=s, bc=bc, bs=bs):
                rows_at = pl.ds(pl.multiple_of(i * step, step), step)
                at = pl.ds(pl.multiple_of(s * 256 + i * step, step), step)
                rc, rs = row_cos[rows_at, :], row_sin[rows_at, :]
                co = rc * bc - rs * bs
                si = rs * bc + rc * bs
                lane = lax.broadcasted_iota(jnp.int32, (step, 128), 1)
                si = jnp.where(lane < 64, -si, si)
                for h in heads:
                    x = acc[at, h * 128 : (h + 1) * 128]
                    y = (x * co + pltpu.roll(x, 64, 1) * si).astype(jnp.bfloat16)
                    if h < 4:
                        Q[h, at, :] = y
                    else:
                        KV[c, 0, at, :] = y
                        KV[c, 1, at, :] = acc[at, 640:768].astype(jnp.bfloat16)
                return carry

            lax.fori_loop(0, 256 // step, rope, 0)

    rotate((4,))
    kv0 = net.send(KV.at[c], m.P)
    kv1 = {s: net.send(KV.at[c], m.Z[s]) for s in SIDES}

    wo0 = {s: net.plan(strip(m.xl, d, s), m.P) for s in SIDES}

    @pl.when(turn == 0)
    def _():
        for s in SIDES:
            net.start(wo0[s])

    acc[:, pl.ds(0, 256)] = columns((m.z, m.zo[1], m.zo[-1], m.z2), 0)

    @pl.when(turn == 1)
    def _():
        along(0, mine, 1).wait_recv()
        along(2, low, 1).start()

    @pl.when(turn == 3)
    def _():
        along(1, mine, -1).wait_recv()
        along(3, high, -1).start()

    @pl.when(turn % 2 == 1)
    def _():
        for s in SIDES:
            net.start(wo1[s])
        for s in SIDES:
            net.start(wo0[s])

    acc[:, pl.ds(256, 256)] = columns((m.z, m.zo[1], m.zo[-1], m.z2), 256)
    rotate((0, 1, 2, 3))

    def bias(s, ctx, half):
        return jnp.where(order[2 * ctx + half] < order[2 * c + s], 0.0, NEG).astype(jnp.float32)

    ones = jnp.ones((512, 128), jnp.bfloat16)
    row = lax.broadcasted_iota(jnp.int32, (256, 256), 0)
    col = lax.broadcasted_iota(jnp.int32, (256, 256), 1)

    def tile(h, s, at, size, ctxs, first, lift):
        q = Q[h, at, :]
        pieces = []
        for ctx, lift_ in zip(ctxs, lift):
            x = lax.dot_general(q, KV[ctx, 0], (((1,), (1,)), ((), ())), preferred_element_type=jnp.float32)
            for half in range(2):
                y = x[:, half * 256 : (half + 1) * 256]
                if first and half == s:
                    y = jnp.where(row >= col, y, NEG)
                pieces.append((y, lift_[s][half]))
        top = None
        for y, b in pieces:
            e = jnp.maximum(y[:, :128], y[:, 128:]) + b
            top = e if top is None else jnp.maximum(top, e)
        new = jnp.broadcast_to(jnp.max(top, axis=1, keepdims=True), (size, 128))
        if not first:
            old = peak[h, at, :]
            new = jnp.maximum(old, new)
        level = new * SCALE
        p = []
        for y, b in pieces:
            down = b - level
            p.append(jnp.exp2(y * SCALE + jnp.concatenate([down, down], axis=1)).astype(jnp.bfloat16))
        part = None
        for i, ctx in enumerate(ctxs):
            value = jnp.concatenate([KV[ctx, 1], ones], axis=1)
            one = jnp.dot(jnp.concatenate(p[2 * i : 2 * i + 2], axis=1), value, preferred_element_type=jnp.float32)
            part = one if part is None else part + one
        if not first:
            factor = jnp.exp2((old - new) * SCALE)
            part = num[h, at, :] * jnp.concatenate([factor, factor], axis=1) + part
        return new, part

    def lifts(ctxs, first=False):
        out = []
        for ctx in ctxs:
            out.append([[jnp.float32(0.0) if first and s == half else bias(s, ctx, half) for half in range(2)] for s in range(2)])
        return out

    def tiles(h, ctxs, first, lift):
        size = 128 if len(ctxs) > 1 else 256
        out = []
        for s in range(2):
            for at in range(s * 256, (s + 1) * 256, size):
                at = pl.ds(at, size)
                out.append((at, tile(h, s, at, size, ctxs, first, lift)))
        return out

    def attend(ctxs, first=False):
        lift = lifts(ctxs, first)
        for h in range(4):
            for at, (new, part) in tiles(h, ctxs, first, lift):
                peak[h, at, :], num[h, at, :] = new, part

    kv2, kv3, kv4, kv5, wo2, wo3, wo4 = {}, {}, {}, {}, {}, {}, {}
    part_of = {1: 0, -1: 1}
    both, early, late = pl.ds(0, 2), pl.ds(0, 320), pl.ds(320, 192)
    attend((c,), True)

    @pl.when(turn == 2)
    def _():
        along(2, low, 1).wait_recv()
        along(3, high, -1).wait_recv()
        for s in SIDES:
            net.start(wo1[s])
        for s in SIDES:
            net.start(wo0[s])


    net.recv(kv0, KV.at[m.c1])
    for s in SIDES:
        kv2[s] = net.send(KV.at[m.c1, both, early], m.Z[s])
    for s in SIDES:
        there = 2 * m.zo[s] + m.xl
        net.recv(kv1[s], KV.at[there])
        kv3[s] = net.send(KV.at[there, part_of[s]], m.Z[s])
        kv5[s] = net.send(KV.at[there, both, late], m.P)
    attend([2 * m.zo[s] + m.xl for s in SIDES])
    for s in SIDES:
        wo3[s] = net.plan(strip(m.xl, m.yo[s], s), m.Y[s])

    def pass_on():
        for s in SIDES:
            net.recv(wo1[s], strip(m.xl, m.yo[s]))
            net.start(wo3[s])

    attend((m.c1,))
    pass_on()
    for s in SIDES:
        there = 2 * m.zo[s] + m.xo
        net.recv(kv2[s], KV.at[there, both, early])
        kv4[s] = net.send(KV.at[there, part_of[s], early], m.Z[s])
    for s in SIDES:
        net.recv(kv3[s], KV.at[2 * m.z2 + m.xl, part_of[s]])
    kv6 = net.send(KV.at[2 * m.z2 + m.xl, both, late], m.P)
    attend((2 * m.z2 + m.xl,))
    for r in SIDES:
        for s in SIDES:
            wo2[r, s] = net.plan(strip(m.xo, d, r), m.Y[s])

    def cross():
        for r in SIDES:
            net.recv(wo0[r], strip(m.xo, d, r))
            for s in SIDES:
                net.start(wo2[r, s])

    cross()
    for s in SIDES:
        net.recv(kv5[s], KV.at[2 * m.zo[s] + m.xo, both, late])
    attend([2 * m.zo[s] + m.xo for s in SIDES])

    for s in SIDES:
        net.recv(kv4[s], KV.at[2 * m.z2 + m.xo, part_of[s], early])
    net.recv(kv6, KV.at[2 * m.z2 + m.xo, both, late])

    last = (2 * m.z2 + m.xo,)
    lift = lifts(last)
    top, bottom = pl.ds(0, 256), pl.ds(256, 256)
    kA = []
    for h in range(4):
        for at, (_, part) in tiles(h, last, False, lift):
            AT[t, h, at, :] = (part[:, :128] / part[:, 128:]).astype(jnp.bfloat16)
        ks = [net.send(AT.at[t, h, pl.ds(s * 256, 256)], (m.P, m.Q)[s], RA.at[s, h]) for s in range(2)]
        ks.append(net.send(AT.at[t, h], m.C))
        kA.append(ks)
    kR = []
    for h in range(4):
        net.recv(kA[h][0], RA.at[0, h])
        a = net.send(RA.at[0, h], m.Q, AT.at[t, h, top])
        net.recv(kA[h][1], RA.at[1, h])
        kR.append((a, net.send(RA.at[1, h], m.P, AT.at[m.t2, h, bottom])))
        if h == 3:
            for s in SIDES:
                net.recv(wo2[s, s], strip(m.xo, m.yo[s], s))
                wo4[s] = net.send(strip(m.xo, m.yo[s], s), m.Y[s])
    kD = []
    for h in range(4):
        net.recv(kR[h][0], AT.at[m.t2, h, top])
        net.recv(kR[h][1], AT.at[m.t2, h, bottom])
        kD.append(net.send(AT.at[m.t2, h], m.C))

    soon = [[(m.xl, d), (m.xl, m.yo[1])], [(m.xl, m.yo[-1]), (m.xl, m.y2)], [(m.xo, d), (m.xo, m.yo[1])]]
    last_two = [(m.xo, m.yo[-1]), (m.xo, m.y2)]

    def product(bs, two):
        left = jnp.concatenate([AT[b, h] for b in bs for h in range(4)], axis=1)
        right = jnp.concatenate(
            [jnp.concatenate([WO[xl * 4 + y, pl.ds(b * 512, 512), :] for b in bs], axis=0) for xl, y in two], axis=1
        )
        return jnp.dot(left, right, preferred_element_type=jnp.float32)

    def project(bs, first=False):
        for two in soon:
            part = product(bs, two)
            for i, (xl, y) in enumerate(two):
                cols = pl.ds(pl.multiple_of((xl * 4 + y) * 128, 128), 128)
                piece = part[:, i * 128 : (i + 1) * 128]
                if first:
                    total[:, cols] = piece
                else:
                    total[:, cols] += piece

    for s in SIDES:
        net.recv(wo3[s], strip(m.xl, m.y2, s))
    net.recv(wo2[-1, 1], strip(m.xo, m.yo[1], -1))
    net.recv(wo2[1, -1], strip(m.xo, m.yo[-1], 1))
    for h in range(4):
        net.recv(kA[h][2], AT.at[m.t1, h])
    project((t, m.t1), True)
    project((m.t2,))
    for h in range(4):
        net.recv(kD[h], AT.at[m.t3, h])
    project((m.t3,))
    for s in SIDES:
        net.recv(wo4[s], strip(m.xo, m.y2, s))
    part = product((t, m.t1, m.t2, m.t3), last_two)
    for i, (xl, y) in enumerate(last_two):
        total[:, pl.ds(pl.multiple_of((xl * 4 + y) * 128, 128), 128)] = part[:, i * 128 : (i + 1) * 128]
    later.wait()

    def close(i, carry):
        at = pl.ds(pl.multiple_of(i * 32, 32), 32)
        branch = total[at, :].astype(jnp.bfloat16)
        out[at, :] = branch
        gap = H[t, at, :].astype(jnp.float32) + branch.astype(jnp.float32) - T[at, :].astype(jnp.float32)
        sq = gap * gap
        for r in range(4):
            for b in range(8):
                carry = carry + sq[r * 8 : (r + 1) * 8, b * 128 : (b + 1) * 128]
        return carry

    part = lax.fori_loop(0, 16, close, jnp.zeros((8, 128), jnp.float32))
    rings = (
        (8, m.xl * 4 + t, lambda i: (2 * m.z + i // 4, i % 4, d)),
        (16, m.z * 4 + d, lambda i: (2 * (i // 4) + m.xl, t, i % 4)),
    )
    for number, (size, me, device) in enumerate(rings):
        LB[number, me] = part
        for j in range(1, size):
            pltpu.make_async_remote_copy(
                src_ref=LB.at[number, me], dst_ref=LB.at[number, me], send_sem=osend.at[5 + number],
                recv_sem=orecv.at[8 + number], device_id=device((me + j) % size), device_id_type=MESH,
            ).start()
        others = LB.at[number, pl.ds(0, size - 1)]
        pltpu.make_async_copy(others, others, orecv.at[8 + number]).wait()
        pltpu.make_async_copy(others, others, osend.at[5 + number]).wait()
        part = LB[number, 0]
        for j in range(1, size):
            part = part + LB[number, j]
    loss_out[0, 0] = jnp.sum(part) / (4 * 4096 * MODEL_WIDTH)
    net.finish()

    @pl.when(t != m.z)
    def _():
        meet(t).wait_send()

    for k, ref, s, when in ((0, mine, 1, 0), (1, mine, -1, 0), (2, low, 1, 1), (3, high, -1, 3)):
        @pl.when(turn == when)
        def _(k=k, ref=ref, s=s):
            along(k, ref, s).wait_send()


def tables():
    freqs = ROPE_BASE ** (-(np.arange(64) * 2.0) / HEAD_SIZE)
    freqs = np.concatenate([freqs, freqs])[None, :]
    rows, blocks = np.arange(256)[:, None] * freqs, np.arange(16)[:, None] * 256 * freqs
    return [f(x).astype(np.float32) for x in (rows, blocks) for f in (np.cos, np.sin)]


def on_device(hidden, target, gain, w_query, w_key, value_matrix, w_out, block_order):
    any_spec = pl.BlockSpec(memory_space=pl.ANY)
    vmem = pl.BlockSpec(memory_space=pltpu.VMEM)
    smem = pl.BlockSpec(memory_space=pltpu.SMEM)
    bf16, f32 = jnp.bfloat16, jnp.float32
    branch, loss = pl.pallas_call(
        layer_kernel,
        out_shape=(pltpu.VMEM((512, 1024), bf16), jax.ShapeDtypeStruct((1, 1), f32)),
        in_specs=[any_spec] * 6 + [vmem, smem, any_spec, any_spec, vmem, vmem],
        out_specs=(vmem, smem),
        scratch_shapes=[
            pltpu.VMEM((4, 512, 1024), bf16),
            pltpu.VMEM((4, 512, 1024), bf16),
            pltpu.VMEM((2, 256, 1024), bf16),
            pltpu.VMEM((8, 4, 128, 768), bf16),
            pltpu.VMEM((512, 768), f32),
            pltpu.VMEM((4, 512, 128), bf16),
            pltpu.VMEM((8, 2, 512, 128), bf16),
            pltpu.VMEM((8, 2048, 128), bf16),
            pltpu.VMEM((4, 4, 512, 128), bf16),
            pltpu.VMEM((2, 4, 256, 128), bf16),
            pltpu.VMEM((4, 512, 256), f32),
            pltpu.VMEM((4, 512, 128), f32),
            pltpu.VMEM((512, 1024), bf16),
            pltpu.VMEM((512, 1024), f32),
            pltpu.VMEM((2, 16, 8, 128), f32),
            pltpu.VMEM((256, 128), f32),
            pltpu.VMEM((256, 128), f32),
            pltpu.SemaphoreType.DMA((POOL,)),
            pltpu.SemaphoreType.DMA((COPIES,)),
            pltpu.SemaphoreType.DMA((8,)),
            pltpu.SemaphoreType.DMA((8,)),
            pltpu.SemaphoreType.DMA((10,)),
        ],
        compiler_params=pltpu.CompilerParams(
            collective_id=0, has_side_effects=True, vmem_limit_bytes=60 * MIB
        ),
        name="layer",
    )(hidden, target, w_query, w_key, value_matrix, w_out, gain[None, :], block_order, *(jnp.asarray(x) for x in tables()))
    return branch[None], loss.reshape(())


def solution(mesh):
    placed = (
        P("dp", "ctx", "tp"), P("dp", "ctx", "tp"), P(), P(("ctx", "dp"), "tp"), P(("ctx", "dp"), "tp"),
        P(("ctx", "dp"), "tp"), P("tp", ("ctx", "dp")), P(),
    )
    return jax.shard_map(
        on_device, mesh=mesh, in_specs=placed, out_specs=(P("dp", "ctx", "tp"), P()), check_vma=False
    )
```

```python
import types

import jax
import jax.numpy as jnp
import numpy as np
from jax import lax
from jax.experimental import pallas as pl
from jax.experimental.pallas import tpu as pltpu
from jax.sharding import PartitionSpec as P

MODEL_WIDTH = 4096
HEAD_SIZE = 128
ROPE_BASE = 500000.0
NEG = -1e30
SCALE = float(np.log2(np.e) / np.sqrt(HEAD_SIZE))
MIB = 1024 * 1024
POOL = 40
COPIES = 120

MESH = pl.DeviceIdType.MESH
SIDES = (1, -1)


def here():
    c, t, d = lax.axis_index("ctx"), lax.axis_index("tp"), lax.axis_index("dp")
    return c, t, d


class Net:
    def __init__(self, send_sems, recv_sems):
        self.send_sems, self.recv_sems = send_sems, recv_sems
        self.started = []

    def copy(self, k, src, dst, dev):
        c, t, d = dev
        return pltpu.make_async_remote_copy(
            src_ref=src,
            dst_ref=dst,
            send_sem=self.send_sems.at[k % POOL],
            recv_sem=self.recv_sems.at[k],
            device_id=(c, t, d),
            device_id_type=MESH,
        )

    def plan(self, ref, dev, dst=None):
        k = len(self.started)
        if k >= POOL:
            self.started[k - POOL][0].wait_send()
        self.started.append((self.copy(k, ref, ref if dst is None else dst, dev), dev))
        return k

    def start(self, k):
        self.started[k][0].start()

    def send(self, ref, dev, dst=None):
        k = self.plan(ref, dev, dst)
        self.start(k)
        return k

    def recv(self, k, ref):
        self.copy(k, ref, ref, self.started[k][1]).wait_recv()

    def finish(self):
        assert len(self.started) <= COPIES
        for copy, _ in self.started[-POOL:]:
            copy.wait_send()


def places():
    c, t, d = here()
    z, xl = c // 2, c % 2
    c1 = c + 1 - 2 * xl
    t1 = t + 1 - 2 * (t % 2)
    t2 = (t + 2) % 4
    t3 = (t1 + 2) % 4
    return types.SimpleNamespace(
        c=c, t=t, d=d, z=z, xl=xl, xo=1 - xl, c1=c1, t1=t1, t2=t2, t3=t3,
        P=(c1, t, d), Q=(c1, t2, d), C=(c, t1, d), R=(c, t2, d), D=(c, t3, d),
        Y={s: (c, t, (d + s) % 4) for s in SIDES},
        Z={s: ((c + 2 * s) % 8, t, d) for s in SIDES},
        yo={s: (d - s) % 4 for s in SIDES},
        zo={s: (z - s) % 4 for s in SIDES},
        y2=(d + 2) % 4, z2=(z + 2) % 4,
    )


def greet(m):
    barrier = pltpu.get_barrier_semaphore()
    others = [m.P, m.Q, m.C, m.R, m.D, m.Y[1], m.Y[-1], m.Z[1], m.Z[-1]]
    for dev in others:
        pl.semaphore_signal(barrier, inc=1, device_id=dev, device_id_type=MESH)
    pl.semaphore_wait(barrier, len(others))


def layer_kernel(
    hid, tgt, wq, wk, wv, wo, gain, order, turn_cos, turn_sin, block_cos, block_sin,
    out, loss_out,
    H, N, RH, W, acc, Q, KV, WO, AT, RA, num, peak, T, total, LB, row_cos, row_sin, ssem, rsem, lsem, osend, orecv, zsend, zrecv,
):
    m = places()
    net = Net(ssem, rsem)
    c, t, d = m.c, m.t, m.d
    local = [
        pltpu.make_async_copy(wq, W.at[c, d, :, pl.ds(0, 512)], lsem.at[0]),
        pltpu.make_async_copy(wk, W.at[c, d, :, pl.ds(512, 128)], lsem.at[1]),
        pltpu.make_async_copy(wv, W.at[c, d, :, pl.ds(640, 128)], lsem.at[2]),
        pltpu.make_async_copy(hid.at[0], H.at[t], lsem.at[3]),
    ]
    for cp in local:
        cp.start()
    later = pltpu.make_async_copy(tgt.at[0], T, lsem.at[4])
    later.start()
    turns = [
        pltpu.make_async_copy(turn_cos, row_cos, lsem.at[6]),
        pltpu.make_async_copy(turn_sin, row_sin, lsem.at[7]),
    ]
    for cp in turns:
        cp.start()
    own_wo = pltpu.make_async_copy(wo, WO.at[m.xl * 4 + d, pl.ds(m.z * 512, 512)], lsem.at[5])
    greet(m)
    for cp in local:
        cp.wait()

    def pair(z):
        return pl.ds(2 * z, 2)

    qa = {1: pl.ds(0, 32), -1: pl.ds(32, 32)}
    qb = {1: pl.ds(64, 32), -1: pl.ds(96, 32)}
    ha, hb = pl.ds(0, 64), pl.ds(64, 64)
    parts = 4
    rows = 256 // parts

    kX = net.send(W.at[c, d], m.P)
    kY1 = {s: net.send(W.at[c, d], m.Y[s]) for s in SIDES}
    kZ1 = {s: net.send(W.at[c, d], m.Z[s]) for s in SIDES}
    kH0 = [net.send(H.at[t, pl.ds(i * rows, rows)], m.P, RH.at[0, pl.ds(i * rows, rows)]) for i in range(parts)]
    kH1 = [net.send(H.at[t, pl.ds(256 + i * rows, rows)], m.Q, RH.at[1, pl.ds(i * rows, rows)]) for i in range(parts)]
    kC = net.send(H.at[t], m.C)

    mine = WO.at[m.xl * 4 + d]
    block = WO.at[m.xl * 4 + d, pl.ds(t * 512, 512)]

    def meet(k):
        return pltpu.make_async_remote_copy(
            src_ref=wo, dst_ref=block, send_sem=osend.at[4], recv_sem=orecv.at[4 + k],
            device_id=(c, m.z, d), device_id_type=MESH,
        )

    @pl.when(t == m.z)
    def _():
        own_wo.start()

    @pl.when(t != m.z)
    def _():
        meet(t).start()

    net.recv(kX, W.at[m.c1, d])
    kY2 = {s: net.send(W.at[m.c1, d], m.Y[s]) for s in SIDES}
    kZ2 = {s: net.send(W.at[m.c1, d], m.Z[s]) for s in SIDES}

    def relay(i):
        net.recv(kH0[i], RH.at[0, pl.ds(i * rows, rows)])
        a = net.send(RH.at[0, pl.ds(i * rows, rows)], m.Q, H.at[t, pl.ds(i * rows, rows)])
        net.recv(kH1[i], RH.at[1, pl.ds(i * rows, rows)])
        b = net.send(RH.at[1, pl.ds(i * rows, rows)], m.P, H.at[m.t2, pl.ds(256 + i * rows, rows)])
        return a, b

    far = []

    def landed(i):
        for k_, lo in ((kF[i][0], i * rows), (kF[i][1], 256 + i * rows)):
            net.recv(k_, H.at[m.t2, pl.ds(lo, rows)])
            far.append((net.send(H.at[m.t2, pl.ds(lo, rows)], m.C), lo))

    kF = []
    fY, fZ, kY3, kZ3, kY4, kZ4 = {}, {}, {}, {}, {}, {}
    for s in SIDES:
        net.recv(kY1[s], W.at[c, m.yo[s]])
        net.recv(kZ1[s], W.at[2 * m.zo[s] + m.xl, d])
    kF.append(relay(0))
    for s in SIDES:
        net.recv(kY2[s], W.at[m.c1, m.yo[s]])
        kY3[s] = net.send(W.at[pair(m.z), m.yo[s], qa[s]], m.Y[s])
        net.recv(kZ2[s], W.at[2 * m.zo[s] + m.xo, d])
        kZ3[s] = net.send(W.at[pair(m.zo[s]), d, qb[s]], m.Z[s])
    for s in SIDES:
        for r in SIDES:
            kZ4[s, r] = net.send(W.at[pair(m.z), m.yo[s], ha], m.Z[r])
            kY4[s, r] = net.send(W.at[pair(m.zo[s]), d, hb], m.Y[r])

    kF += [relay(1), relay(2)]
    kY6, kZ6 = {}, {}
    for s in SIDES:
        net.recv(kY3[s], W.at[pair(m.z), m.y2, qa[s]])
        net.recv(kZ3[s], W.at[pair(m.z2), d, qb[s]])
    for r in SIDES:
        kZ6[r] = net.send(W.at[pair(m.z), m.y2, ha], m.Z[r])
        kY6[r] = net.send(W.at[pair(m.z2), d, hb], m.Y[r])
    for s in SIDES:
        fZ[s, "own"] = net.send(W.at[pair(m.zo[s]), d, qa[s]], m.Z[s])
        fY[s, "own"] = net.send(W.at[pair(m.z), m.yo[s], qb[s]], m.Y[s])
    kF.append(relay(3))
    for s in SIDES:
        for r in SIDES:
            net.recv(kZ4[s, r], W.at[pair(m.zo[r]), m.yo[s], ha])
            fZ[r, s] = net.send(W.at[pair(m.zo[r]), m.yo[s], qa[r]], m.Z[r])
            net.recv(kY4[s, r], W.at[pair(m.zo[s]), m.yo[r], hb])
            fY[r, s] = net.send(W.at[pair(m.zo[s]), m.yo[r], qb[r]], m.Y[r])
    landed(0)
    landed(1)
    landed(2)
    landed(3)
    for r in SIDES:
        net.recv(kZ6[r], W.at[pair(m.zo[r]), m.y2, ha])
        fZ[r, "far"] = net.send(W.at[pair(m.zo[r]), m.y2, qa[r]], m.Z[r])
        net.recv(kY6[r], W.at[pair(m.z2), m.yo[r], hb])
        fY[r, "far"] = net.send(W.at[pair(m.z2), m.yo[r], qb[r]], m.Y[r])
    turn = (m.z - t + 4) % 4

    def along(k, ref, s):
        return pltpu.make_async_remote_copy(
            src_ref=ref, dst_ref=ref, send_sem=zsend.at[k], recv_sem=zrecv.at[k],
            device_id=m.Z[s], device_id_type=MESH,
        )

    low = WO.at[m.xl * 4 + d, pl.ds(0, 1024)]
    high = WO.at[m.xl * 4 + d, pl.ds(1024, 1024)]

    @pl.when(turn == 0)
    def _():
        own_wo.wait()
        for k in range(4):
            @pl.when(k != t)
            def _(k=k):
                there = WO.at[m.xl * 4 + d, pl.ds(k * 512, 512)]
                pltpu.make_async_remote_copy(
                    src_ref=there, dst_ref=there, send_sem=osend.at[4], recv_sem=orecv.at[4 + k],
                    device_id=(c, m.z, d), device_id_type=MESH,
                ).wait_recv()

        along(0, low, 1).start()
        along(1, high, -1).start()
        along(4, high, 1).start()
        along(5, low, -1).start()

    def strip(xl, y, s=None):
        return WO.at[xl * 4 + y] if s is None else WO.at[xl * 4 + y, pl.ds(0 if s == 1 else 1024, 1024)]

    wo1 = {s: net.plan(mine, m.Y[s]) for s in SIDES}

    @pl.when(turn == 0)
    def _():
        for s in SIDES:
            net.start(wo1[s])

    net.recv(kC, H.at[m.t1])
    for k, lo in far:
        net.recv(k, H.at[m.t3, pl.ds(lo, rows)])


    step = 64

    def norm(i, carry):
        at = pl.ds(pl.multiple_of(i * step, step), step)
        total = jnp.zeros((step, 1), jnp.float32)
        for b in range(4):
            x = H[b, at, :].astype(jnp.float32)
            total = total + jnp.sum(x * x, axis=1, keepdims=True)
        scale = lax.rsqrt(total * (1.0 / MODEL_WIDTH) + 1e-05)
        for b in range(4):
            x = H[b, at, :].astype(jnp.float32)
            g = gain[:, b * 1024 : (b + 1) * 1024]
            N[b, at, :] = (x * scale * g).astype(jnp.bfloat16)
        return carry

    lax.fori_loop(0, 512 // step, norm, 0)

    def columns(zs, lo):
        cols = pl.ds(lo, 256)
        sums = None
        for z in zs:
            w = W[pair(z), :, :, cols].reshape(1024, 256)
            part = jnp.dot(N[z], w, preferred_element_type=jnp.float32)
            sums = part if sums is None else sums + part
        return sums

    for r in SIDES:
        net.recv(fY[r, "own"], W.at[pair(m.z), m.y2, qb[r]])
        for s in SIDES:
            net.recv(fY[r, s], W.at[pair(m.zo[s]), m.y2, qb[r]])
    acc[:, pl.ds(512, 256)] = columns((m.z, m.zo[1], m.zo[-1]), 512)

    for r in SIDES:
        net.recv(fZ[r, "own"], W.at[pair(m.z2), d, qa[r]])
        for s in SIDES:
            net.recv(fZ[r, s], W.at[pair(m.z2), m.yo[s], qa[r]])
        net.recv(fZ[r, "far"], W.at[pair(m.z2), m.y2, qa[r]])
        net.recv(fY[r, "far"], W.at[pair(m.z2), m.y2, qb[r]])
    acc[:, pl.ds(512, 256)] += columns((m.z2,), 512)
    for cp in turns:
        cp.wait()

    def rotate(heads):
        for s in range(2):
            where = order[2 * c + s]
            bc, bs = block_cos[pl.ds(where, 1), :], block_sin[pl.ds(where, 1), :]

            def rope(i, carry, s=s, bc=bc, bs=bs):
                rows_at = pl.ds(pl.multiple_of(i * step, step), step)
                at = pl.ds(pl.multiple_of(s * 256 + i * step, step), step)
                rc, rs = row_cos[rows_at, :], row_sin[rows_at, :]
                co = rc * bc - rs * bs
                si = rs * bc + rc * bs
                lane = lax.broadcasted_iota(jnp.int32, (step, 128), 1)
                si = jnp.where(lane < 64, -si, si)
                for h in heads:
                    x = acc[at, h * 128 : (h + 1) * 128]
                    y = (x * co + pltpu.roll(x, 64, 1) * si).astype(jnp.bfloat16)
                    if h < 4:
                        Q[h, at, :] = y
                    else:
                        KV[c, 0, at, :] = y
                        KV[c, 1, at, :] = acc[at, 640:768].astype(jnp.bfloat16)
                return carry

            lax.fori_loop(0, 256 // step, rope, 0)

    rotate((4,))
    @pl.when(turn == 1)
    def _():
        along(0, low, 1).wait_recv()
        along(2, low, 1).start()

    @pl.when(turn == 3)
    def _():
        along(1, high, -1).wait_recv()
        along(3, high, -1).start()

    kv0 = net.send(KV.at[c], m.P)
    kv1 = {s: net.send(KV.at[c], m.Z[s]) for s in SIDES}

    wo0 = {s: net.plan(strip(m.xl, d, s), m.P) for s in SIDES}

    @pl.when(turn == 0)
    def _():
        for s in SIDES:
            net.start(wo0[s])

    acc[:, pl.ds(0, 256)] = columns((m.z, m.zo[1], m.zo[-1], m.z2), 0)

    acc[:, pl.ds(256, 256)] = columns((m.z, m.zo[1], m.zo[-1], m.z2), 256)

    @pl.when(turn == 1)
    def _():
        along(4, high, 1).wait_recv()

    @pl.when(turn == 3)
    def _():
        along(5, low, -1).wait_recv()

    @pl.when(turn % 2 == 1)
    def _():
        for s in SIDES:
            net.start(wo1[s])
        for s in SIDES:
            net.start(wo0[s])

    rotate((0, 1, 2, 3))

    def bias(s, ctx, half):
        return jnp.where(order[2 * ctx + half] < order[2 * c + s], 0.0, NEG).astype(jnp.float32)

    ones = jnp.ones((512, 128), jnp.bfloat16)
    row = lax.broadcasted_iota(jnp.int32, (256, 256), 0)
    col = lax.broadcasted_iota(jnp.int32, (256, 256), 1)

    def tile(h, s, at, size, ctxs, first, lift):
        q = Q[h, at, :]
        pieces = []
        for ctx, lift_ in zip(ctxs, lift):
            x = lax.dot_general(q, KV[ctx, 0], (((1,), (1,)), ((), ())), preferred_element_type=jnp.float32)
            for half in range(2):
                y = x[:, half * 256 : (half + 1) * 256]
                if first and half == s:
                    y = jnp.where(row >= col, y, NEG)
                pieces.append((y, lift_[s][half]))
        top = None
        for y, b in pieces:
            e = jnp.maximum(y[:, :128], y[:, 128:]) + b
            top = e if top is None else jnp.maximum(top, e)
        new = jnp.broadcast_to(jnp.max(top, axis=1, keepdims=True), (size, 128))
        if not first:
            old = peak[h, at, :]
            new = jnp.maximum(old, new)
        level = new * SCALE
        p = []
        for y, b in pieces:
            down = b - level
            p.append(jnp.exp2(y * SCALE + jnp.concatenate([down, down], axis=1)).astype(jnp.bfloat16))
        part = None
        for i, ctx in enumerate(ctxs):
            value = jnp.concatenate([KV[ctx, 1], ones], axis=1)
            one = jnp.dot(jnp.concatenate(p[2 * i : 2 * i + 2], axis=1), value, preferred_element_type=jnp.float32)
            part = one if part is None else part + one
        if not first:
            factor = jnp.exp2((old - new) * SCALE)
            part = num[h, at, :] * jnp.concatenate([factor, factor], axis=1) + part
        return new, part

    def lifts(ctxs, first=False):
        out = []
        for ctx in ctxs:
            out.append([[jnp.float32(0.0) if first and s == half else bias(s, ctx, half) for half in range(2)] for s in range(2)])
        return out

    def tiles(h, ctxs, first, lift):
        size = 128 if len(ctxs) > 1 else 256
        out = []
        for s in range(2):
            for at in range(s * 256, (s + 1) * 256, size):
                at = pl.ds(at, size)
                out.append((at, tile(h, s, at, size, ctxs, first, lift)))
        return out

    def attend(ctxs, first=False, between=None):
        lift = lifts(ctxs, first)
        for h in range(4):
            if between is not None and h == 2:
                between()
            for at, (new, part) in tiles(h, ctxs, first, lift):
                peak[h, at, :], num[h, at, :] = new, part

    kv2, kv3, kv4, kv5, wo2, wo3, wo4 = {}, {}, {}, {}, {}, {}, {}
    part_of = {1: 0, -1: 1}
    both, early, late = pl.ds(0, 2), pl.ds(0, 320), pl.ds(320, 192)
    def to_z():
        net.recv(kv0, KV.at[m.c1])
        for s in SIDES:
            kv2[s] = net.send(KV.at[m.c1, both, early], m.Z[s])

        @pl.when(turn == 2)
        def _():
            along(2, low, 1).wait_recv()
            along(3, high, -1).wait_recv()
            for s in SIDES:
                net.start(wo1[s])
            for s in SIDES:
                net.start(wo0[s])

    attend((c,), True, to_z)

    for s in SIDES:
        there = 2 * m.zo[s] + m.xl
        net.recv(kv1[s], KV.at[there])
        kv3[s] = net.send(KV.at[there, part_of[s]], m.Z[s])
        kv5[s] = net.send(KV.at[there, both, late], m.P)
    attend([2 * m.zo[s] + m.xl for s in SIDES])
    for s in SIDES:
        wo3[s] = net.plan(strip(m.xl, m.yo[s], s), m.Y[s])

    def pass_on():
        for s in SIDES:
            net.recv(wo1[s], strip(m.xl, m.yo[s]))
            net.start(wo3[s])

    @pl.when(turn == 0)
    def _():
        pass_on()

    attend((m.c1,))
    for s in SIDES:
        there = 2 * m.zo[s] + m.xo
        net.recv(kv2[s], KV.at[there, both, early])
        kv4[s] = net.send(KV.at[there, part_of[s], early], m.Z[s])
    for s in SIDES:
        net.recv(kv3[s], KV.at[2 * m.z2 + m.xl, part_of[s]])
    kv6 = net.send(KV.at[2 * m.z2 + m.xl, both, late], m.P)
    for r in SIDES:
        for s in SIDES:
            wo2[r, s] = net.plan(strip(m.xo, d, r), m.Y[s])

    def cross():
        for r in SIDES:
            net.recv(wo0[r], strip(m.xo, d, r))
            for s in SIDES:
                net.start(wo2[r, s])

    @pl.when(turn % 2 == 1)
    def _():
        pass_on()

    attend((2 * m.z2 + m.xl,))

    @pl.when(turn != 2)
    def _():
        cross()

    for s in SIDES:
        net.recv(kv5[s], KV.at[2 * m.zo[s] + m.xo, both, late])
    attend([2 * m.zo[s] + m.xo for s in SIDES])

    @pl.when(turn == 2)
    def _():
        pass_on()
        cross()


    for s in SIDES:
        net.recv(kv4[s], KV.at[2 * m.z2 + m.xo, part_of[s], early])
    net.recv(kv6, KV.at[2 * m.z2 + m.xo, both, late])

    last = (2 * m.z2 + m.xo,)
    lift = lifts(last)
    top, bottom = pl.ds(0, 256), pl.ds(256, 256)
    kA = []
    for h in range(4):
        for at, (_, part) in tiles(h, last, False, lift):
            AT[t, h, at, :] = (part[:, :128] / part[:, 128:]).astype(jnp.bfloat16)
        ks = [net.send(AT.at[t, h, pl.ds(s * 256, 256)], (m.P, m.Q)[s], RA.at[s, h]) for s in range(2)]
        ks.append(net.send(AT.at[t, h], m.C))
        kA.append(ks)
    for s in SIDES:
        wo4[s] = net.plan(strip(m.xo, m.yo[s], s), m.Y[s])

    def hop(now):
        @pl.when(now)
        def _():
            for s in SIDES:
                net.recv(wo2[s, s], strip(m.xo, m.yo[s], s))
                net.start(wo4[s])

    hop(turn == 0)
    kR = []
    for h in range(4):
        net.recv(kA[h][0], RA.at[0, h])
        a = net.send(RA.at[0, h], m.Q, AT.at[t, h, top])
        net.recv(kA[h][1], RA.at[1, h])
        kR.append((a, net.send(RA.at[1, h], m.P, AT.at[m.t2, h, bottom])))
        if h == 1:
            hop(turn % 2 == 1)
    hop(turn == 2)
    kD = []
    for h in range(4):
        net.recv(kR[h][0], AT.at[m.t2, h, top])
        net.recv(kR[h][1], AT.at[m.t2, h, bottom])
        kD.append(net.send(AT.at[m.t2, h], m.C))

    soon = [[(m.xl, d), (m.xl, m.yo[1])], [(m.xl, m.yo[-1]), (m.xl, m.y2)], [(m.xo, d), (m.xo, m.yo[1])]]
    last_two = [(m.xo, m.yo[-1]), (m.xo, m.y2)]

    def product(bs, two):
        left = jnp.concatenate([AT[b, h] for b in bs for h in range(4)], axis=1)
        right = jnp.concatenate(
            [jnp.concatenate([WO[xl * 4 + y, pl.ds(b * 512, 512), :] for b in bs], axis=0) for xl, y in two], axis=1
        )
        return jnp.dot(left, right, preferred_element_type=jnp.float32)

    def project(bs, first=False):
        for two in soon:
            part = product(bs, two)
            for i, (xl, y) in enumerate(two):
                cols = pl.ds(pl.multiple_of((xl * 4 + y) * 128, 128), 128)
                piece = part[:, i * 128 : (i + 1) * 128]
                if first:
                    total[:, cols] = piece
                else:
                    total[:, cols] += piece

    for s in SIDES:
        net.recv(wo3[s], strip(m.xl, m.y2, s))
    net.recv(wo2[-1, 1], strip(m.xo, m.yo[1], -1))
    net.recv(wo2[1, -1], strip(m.xo, m.yo[-1], 1))
    for h in range(4):
        net.recv(kA[h][2], AT.at[m.t1, h])
    project((t, m.t1), True)
    project((m.t2,))
    for h in range(4):
        net.recv(kD[h], AT.at[m.t3, h])
    project((m.t3,))
    for s in SIDES:
        net.recv(wo4[s], strip(m.xo, m.y2, s))
    part = product((t, m.t1, m.t2, m.t3), last_two)
    for i, (xl, y) in enumerate(last_two):
        total[:, pl.ds(pl.multiple_of((xl * 4 + y) * 128, 128), 128)] = part[:, i * 128 : (i + 1) * 128]
    later.wait()

    def close(i, carry):
        at = pl.ds(pl.multiple_of(i * 32, 32), 32)
        branch = total[at, :].astype(jnp.bfloat16)
        out[at, :] = branch
        gap = H[t, at, :].astype(jnp.float32) + branch.astype(jnp.float32) - T[at, :].astype(jnp.float32)
        sq = gap * gap
        for r in range(4):
            for b in range(8):
                carry = carry + sq[r * 8 : (r + 1) * 8, b * 128 : (b + 1) * 128]
        return carry

    part = lax.fori_loop(0, 16, close, jnp.zeros((8, 128), jnp.float32))
    rings = (
        (8, m.xl * 4 + t, lambda i: (2 * m.z + i // 4, i % 4, d)),
        (16, m.z * 4 + d, lambda i: (2 * (i // 4) + m.xl, t, i % 4)),
    )
    for number, (size, me, device) in enumerate(rings):
        LB[number, me] = part
        for j in range(1, size):
            pltpu.make_async_remote_copy(
                src_ref=LB.at[number, me], dst_ref=LB.at[number, me], send_sem=osend.at[5 + number],
                recv_sem=orecv.at[8 + number], device_id=device((me + j) % size), device_id_type=MESH,
            ).start()
        others = LB.at[number, pl.ds(0, size - 1)]
        pltpu.make_async_copy(others, others, orecv.at[8 + number]).wait()
        pltpu.make_async_copy(others, others, osend.at[5 + number]).wait()
        part = LB[number, 0]
        for j in range(1, size):
            part = part + LB[number, j]
    loss_out[0, 0] = jnp.sum(part) / (4 * 4096 * MODEL_WIDTH)
    net.finish()

    @pl.when(t != m.z)
    def _():
        meet(t).wait_send()

    for k, ref, s, when in ((0, low, 1, 0), (1, high, -1, 0), (4, high, 1, 0), (5, low, -1, 0), (2, low, 1, 1), (3, high, -1, 3)):
        @pl.when(turn == when)
        def _(k=k, ref=ref, s=s):
            along(k, ref, s).wait_send()


def tables():
    freqs = ROPE_BASE ** (-(np.arange(64) * 2.0) / HEAD_SIZE)
    freqs = np.concatenate([freqs, freqs])[None, :]
    rows, blocks = np.arange(256)[:, None] * freqs, np.arange(16)[:, None] * 256 * freqs
    return [f(x).astype(np.float32) for x in (rows, blocks) for f in (np.cos, np.sin)]


def on_device(hidden, target, gain, w_query, w_key, value_matrix, w_out, block_order):
    any_spec = pl.BlockSpec(memory_space=pl.ANY)
    vmem = pl.BlockSpec(memory_space=pltpu.VMEM)
    smem = pl.BlockSpec(memory_space=pltpu.SMEM)
    bf16, f32 = jnp.bfloat16, jnp.float32
    branch, loss = pl.pallas_call(
        layer_kernel,
        out_shape=(pltpu.VMEM((512, 1024), bf16), jax.ShapeDtypeStruct((1, 1), f32)),
        in_specs=[any_spec] * 6 + [vmem, smem, any_spec, any_spec, vmem, vmem],
        out_specs=(vmem, smem),
        scratch_shapes=[
            pltpu.VMEM((4, 512, 1024), bf16),
            pltpu.VMEM((4, 512, 1024), bf16),
            pltpu.VMEM((2, 256, 1024), bf16),
            pltpu.VMEM((8, 4, 128, 768), bf16),
            pltpu.VMEM((512, 768), f32),
            pltpu.VMEM((4, 512, 128), bf16),
            pltpu.VMEM((8, 2, 512, 128), bf16),
            pltpu.VMEM((8, 2048, 128), bf16),
            pltpu.VMEM((4, 4, 512, 128), bf16),
            pltpu.VMEM((2, 4, 256, 128), bf16),
            pltpu.VMEM((4, 512, 256), f32),
            pltpu.VMEM((4, 512, 128), f32),
            pltpu.VMEM((512, 1024), bf16),
            pltpu.VMEM((512, 1024), f32),
            pltpu.VMEM((2, 16, 8, 128), f32),
            pltpu.VMEM((256, 128), f32),
            pltpu.VMEM((256, 128), f32),
            pltpu.SemaphoreType.DMA((POOL,)),
            pltpu.SemaphoreType.DMA((COPIES,)),
            pltpu.SemaphoreType.DMA((8,)),
            pltpu.SemaphoreType.DMA((8,)),
            pltpu.SemaphoreType.DMA((10,)),
            pltpu.SemaphoreType.DMA((6,)),
            pltpu.SemaphoreType.DMA((6,)),
        ],
        compiler_params=pltpu.CompilerParams(
            collective_id=0, has_side_effects=True, vmem_limit_bytes=60 * MIB
        ),
        name="layer",
    )(hidden, target, w_query, w_key, value_matrix, w_out, gain[None, :], block_order, *(jnp.asarray(x) for x in tables()))
    return branch[None], loss.reshape(())


def solution(mesh):
    placed = (
        P("dp", "ctx", "tp"), P("dp", "ctx", "tp"), P(), P(("ctx", "dp"), "tp"), P(("ctx", "dp"), "tp"),
        P(("ctx", "dp"), "tp"), P("tp", ("ctx", "dp")), P(),
    )
    return jax.shard_map(
        on_device, mesh=mesh, in_specs=placed, out_specs=(P("dp", "ctx", "tp"), P()), check_vma=False
    )
```

```python
import types

import jax
import jax.numpy as jnp
import numpy as np
from jax import lax
from jax.experimental import pallas as pl
from jax.experimental.pallas import tpu as pltpu
from jax.sharding import PartitionSpec as P

MODEL_WIDTH = 4096
HEAD_SIZE = 128
ROPE_BASE = 500000.0
NEG = -1e30
SCALE = float(np.log2(np.e) / np.sqrt(HEAD_SIZE))
MIB = 1024 * 1024
POOL = 64
COPIES = 112

MESH = pl.DeviceIdType.MESH
SIDES = (1, -1)


def here():
    c, t, d = lax.axis_index("ctx"), lax.axis_index("tp"), lax.axis_index("dp")
    return c, t, d


class Net:
    def __init__(self, send_sems, recv_sems):
        self.send_sems, self.recv_sems = send_sems, recv_sems
        self.started = []

    def copy(self, k, src, dst, dev):
        c, t, d = dev
        return pltpu.make_async_remote_copy(
            src_ref=src,
            dst_ref=dst,
            send_sem=self.send_sems.at[k % POOL],
            recv_sem=self.recv_sems.at[k],
            device_id=(c, t, d),
            device_id_type=MESH,
        )

    def plan(self, ref, dev, dst=None):
        k = len(self.started)
        if k >= POOL:
            self.started[k - POOL][0].wait_send()
        self.started.append((self.copy(k, ref, ref if dst is None else dst, dev), dev))
        return k

    def start(self, k):
        self.started[k][0].start()

    def send(self, ref, dev, dst=None):
        k = self.plan(ref, dev, dst)
        self.start(k)
        return k

    def recv(self, k, ref):
        self.copy(k, ref, ref, self.started[k][1]).wait_recv()

    def finish(self):
        assert len(self.started) <= COPIES
        for copy, _ in self.started[-POOL:]:
            copy.wait_send()


def places():
    c, t, d = here()
    z, xl = c // 2, c % 2
    c1 = c + 1 - 2 * xl
    t1 = t + 1 - 2 * (t % 2)
    t2 = (t + 2) % 4
    t3 = (t1 + 2) % 4
    return types.SimpleNamespace(
        c=c, t=t, d=d, z=z, xl=xl, xo=1 - xl, c1=c1, t1=t1, t2=t2, t3=t3,
        P=(c1, t, d), Q=(c1, t2, d), C=(c, t1, d), R=(c, t2, d), D=(c, t3, d),
        Y={s: (c, t, (d + s) % 4) for s in SIDES},
        Z={s: ((c + 2 * s) % 8, t, d) for s in SIDES},
        yo={s: (d - s) % 4 for s in SIDES},
        zo={s: (z - s) % 4 for s in SIDES},
        y2=(d + 2) % 4, z2=(z + 2) % 4,
    )


def greet(m):
    barrier = pltpu.get_barrier_semaphore()
    others = [m.P, m.Q, m.C, m.R, m.D, m.Y[1], m.Y[-1], m.Z[1], m.Z[-1]]
    for dev in others:
        pl.semaphore_signal(barrier, inc=1, device_id=dev, device_id_type=MESH)
    pl.semaphore_wait(barrier, len(others))


def layer_kernel(
    hid, tgt, wq, wk, wv, wo, gain, order, turn_cos, turn_sin, block_cos, block_sin,
    out, loss_out,
    H, N, RH, W, acc, Q, KV, WO, AT, RA, num, peak, T, total, LB, row_cos, row_sin, ssem, rsem, lsem, osend, orecv, zsend, zrecv,
):
    m = places()
    net = Net(ssem, rsem)
    c, t, d = m.c, m.t, m.d
    local = [
        pltpu.make_async_copy(wq, W.at[c, d, :, pl.ds(0, 512)], lsem.at[0]),
        pltpu.make_async_copy(wk, W.at[c, d, :, pl.ds(512, 128)], lsem.at[1]),
        pltpu.make_async_copy(wv, W.at[c, d, :, pl.ds(640, 128)], lsem.at[2]),
        pltpu.make_async_copy(hid.at[0], H.at[t], lsem.at[3]),
    ]
    for cp in local:
        cp.start()
    later = pltpu.make_async_copy(tgt.at[0], T, lsem.at[4])
    later.start()
    turns = [
        pltpu.make_async_copy(turn_cos, row_cos, lsem.at[6]),
        pltpu.make_async_copy(turn_sin, row_sin, lsem.at[7]),
    ]
    for cp in turns:
        cp.start()
    own_wo = pltpu.make_async_copy(wo, WO.at[m.xl * 4 + d, pl.ds(m.z * 512, 512)], lsem.at[5])
    greet(m)
    for cp in local:
        cp.wait()

    def pair(z):
        return pl.ds(2 * z, 2)

    qa = {1: pl.ds(0, 32), -1: pl.ds(32, 32)}
    qb = {1: pl.ds(64, 32), -1: pl.ds(96, 32)}
    ha, hb = pl.ds(0, 64), pl.ds(64, 64)
    parts = 4
    rows = 256 // parts

    kX = net.send(W.at[c, d], m.P)
    kY1 = {s: net.send(W.at[c, d], m.Y[s]) for s in SIDES}
    kZ1 = {s: net.send(W.at[c, d], m.Z[s]) for s in SIDES}
    kH0 = [net.send(H.at[t, pl.ds(i * rows, rows)], m.P, RH.at[0, pl.ds(i * rows, rows)]) for i in range(parts)]
    kH1 = [net.send(H.at[t, pl.ds(256 + i * rows, rows)], m.Q, RH.at[1, pl.ds(i * rows, rows)]) for i in range(parts)]
    kC = net.send(H.at[t], m.C)

    mine = WO.at[m.xl * 4 + d]
    block = WO.at[m.xl * 4 + d, pl.ds(t * 512, 512)]

    def meet(k):
        return pltpu.make_async_remote_copy(
            src_ref=wo, dst_ref=block, send_sem=osend.at[4], recv_sem=orecv.at[4 + k],
            device_id=(c, m.z, d), device_id_type=MESH,
        )

    @pl.when(t == m.z)
    def _():
        own_wo.start()

    @pl.when(t != m.z)
    def _():
        meet(t).start()

    net.recv(kX, W.at[m.c1, d])
    kY2 = {s: net.send(W.at[m.c1, d], m.Y[s]) for s in SIDES}
    kZ2 = {s: net.send(W.at[m.c1, d], m.Z[s]) for s in SIDES}

    def relay(i):
        net.recv(kH0[i], RH.at[0, pl.ds(i * rows, rows)])
        a = net.send(RH.at[0, pl.ds(i * rows, rows)], m.Q, H.at[t, pl.ds(i * rows, rows)])
        net.recv(kH1[i], RH.at[1, pl.ds(i * rows, rows)])
        b = net.send(RH.at[1, pl.ds(i * rows, rows)], m.P, H.at[m.t2, pl.ds(256 + i * rows, rows)])
        return a, b

    far = []

    def landed(i):
        for k_, lo in ((kF[i][0], i * rows), (kF[i][1], 256 + i * rows)):
            net.recv(k_, H.at[m.t2, pl.ds(lo, rows)])
            far.append((net.send(H.at[m.t2, pl.ds(lo, rows)], m.C), lo))

    kF = []
    fY, fZ, kY3, kZ3, kY4, kZ4 = {}, {}, {}, {}, {}, {}
    for s in SIDES:
        net.recv(kY1[s], W.at[c, m.yo[s]])
        net.recv(kZ1[s], W.at[2 * m.zo[s] + m.xl, d])
    kF.append(relay(0))
    for s in SIDES:
        net.recv(kY2[s], W.at[m.c1, m.yo[s]])
        kY3[s] = net.send(W.at[pair(m.z), m.yo[s], qa[s]], m.Y[s])
        net.recv(kZ2[s], W.at[2 * m.zo[s] + m.xo, d])
        kZ3[s] = net.send(W.at[pair(m.zo[s]), d, qb[s]], m.Z[s])
    for s in SIDES:
        for r in SIDES:
            kZ4[s, r] = net.send(W.at[pair(m.z), m.yo[s], ha], m.Z[r])
            kY4[s, r] = net.send(W.at[pair(m.zo[s]), d, hb], m.Y[r])

    kF += [relay(1), relay(2)]
    kY6, kZ6 = {}, {}
    for s in SIDES:
        net.recv(kY3[s], W.at[pair(m.z), m.y2, qa[s]])
        net.recv(kZ3[s], W.at[pair(m.z2), d, qb[s]])
    for r in SIDES:
        kZ6[r] = net.send(W.at[pair(m.z), m.y2, ha], m.Z[r])
        kY6[r] = net.send(W.at[pair(m.z2), d, hb], m.Y[r])
    for s in SIDES:
        fZ[s, "own"] = net.send(W.at[pair(m.zo[s]), d, qa[s]], m.Z[s])
        fY[s, "own"] = net.send(W.at[pair(m.z), m.yo[s], qb[s]], m.Y[s])
    kF.append(relay(3))
    for s in SIDES:
        for r in SIDES:
            net.recv(kZ4[s, r], W.at[pair(m.zo[r]), m.yo[s], ha])
            fZ[r, s] = net.send(W.at[pair(m.zo[r]), m.yo[s], qa[r]], m.Z[r])
            net.recv(kY4[s, r], W.at[pair(m.zo[s]), m.yo[r], hb])
            fY[r, s] = net.send(W.at[pair(m.zo[s]), m.yo[r], qb[r]], m.Y[r])
    landed(0)
    landed(1)
    landed(2)
    landed(3)
    for r in SIDES:
        net.recv(kZ6[r], W.at[pair(m.zo[r]), m.y2, ha])
        fZ[r, "far"] = net.send(W.at[pair(m.zo[r]), m.y2, qa[r]], m.Z[r])
        net.recv(kY6[r], W.at[pair(m.z2), m.yo[r], hb])
        fY[r, "far"] = net.send(W.at[pair(m.z2), m.yo[r], qb[r]], m.Y[r])
    turn = (m.z - t + 4) % 4

    def along(k, ref, s):
        return pltpu.make_async_remote_copy(
            src_ref=ref, dst_ref=ref, send_sem=zsend.at[k], recv_sem=zrecv.at[k],
            device_id=m.Z[s], device_id_type=MESH,
        )

    low = WO.at[m.xl * 4 + d, pl.ds(0, 1024)]
    high = WO.at[m.xl * 4 + d, pl.ds(1024, 1024)]

    @pl.when(turn == 0)
    def _():
        own_wo.wait()
        for k in range(4):
            @pl.when(k != t)
            def _(k=k):
                there = WO.at[m.xl * 4 + d, pl.ds(k * 512, 512)]
                pltpu.make_async_remote_copy(
                    src_ref=there, dst_ref=there, send_sem=osend.at[4], recv_sem=orecv.at[4 + k],
                    device_id=(c, m.z, d), device_id_type=MESH,
                ).wait_recv()

        along(0, low, 1).start()
        along(1, high, -1).start()
        along(4, high, 1).start()
        along(5, low, -1).start()

    def strip(xl, y, s=None):
        return WO.at[xl * 4 + y] if s is None else WO.at[xl * 4 + y, pl.ds(0 if s == 1 else 1024, 1024)]

    wo1 = {s: net.plan(mine, m.Y[s]) for s in SIDES}

    @pl.when(turn == 0)
    def _():
        for s in SIDES:
            net.start(wo1[s])

    net.recv(kC, H.at[m.t1])
    for k, lo in far:
        net.recv(k, H.at[m.t3, pl.ds(lo, rows)])


    step = 64

    def norm(i, carry):
        at = pl.ds(pl.multiple_of(i * step, step), step)
        total = jnp.zeros((step, 1), jnp.float32)
        for b in range(4):
            x = H[b, at, :].astype(jnp.float32)
            total = total + jnp.sum(x * x, axis=1, keepdims=True)
        scale = lax.rsqrt(total * (1.0 / MODEL_WIDTH) + 1e-05)
        for b in range(4):
            x = H[b, at, :].astype(jnp.float32)
            g = gain[:, b * 1024 : (b + 1) * 1024]
            N[b, at, :] = (x * scale * g).astype(jnp.bfloat16)
        return carry

    lax.fori_loop(0, 512 // step, norm, 0)

    def columns(zs, lo):
        cols = pl.ds(lo, 256)
        sums = None
        for z in zs:
            w = W[pair(z), :, :, cols].reshape(1024, 256)
            part = jnp.dot(N[z], w, preferred_element_type=jnp.float32)
            sums = part if sums is None else sums + part
        return sums

    for r in SIDES:
        net.recv(fY[r, "own"], W.at[pair(m.z), m.y2, qb[r]])
        for s in SIDES:
            net.recv(fY[r, s], W.at[pair(m.zo[s]), m.y2, qb[r]])
    acc[:, pl.ds(512, 256)] = columns((m.z, m.zo[1], m.zo[-1]), 512)

    for r in SIDES:
        net.recv(fZ[r, "own"], W.at[pair(m.z2), d, qa[r]])
        for s in SIDES:
            net.recv(fZ[r, s], W.at[pair(m.z2), m.yo[s], qa[r]])
        net.recv(fZ[r, "far"], W.at[pair(m.z2), m.y2, qa[r]])
        net.recv(fY[r, "far"], W.at[pair(m.z2), m.y2, qb[r]])
    acc[:, pl.ds(512, 256)] += columns((m.z2,), 512)
    for cp in turns:
        cp.wait()

    def rotate(heads):
        for s in range(2):
            where = order[2 * c + s]
            bc, bs = block_cos[pl.ds(where, 1), :], block_sin[pl.ds(where, 1), :]

            def rope(i, carry, s=s, bc=bc, bs=bs):
                rows_at = pl.ds(pl.multiple_of(i * step, step), step)
                at = pl.ds(pl.multiple_of(s * 256 + i * step, step), step)
                rc, rs = row_cos[rows_at, :], row_sin[rows_at, :]
                co = rc * bc - rs * bs
                si = rs * bc + rc * bs
                lane = lax.broadcasted_iota(jnp.int32, (step, 128), 1)
                si = jnp.where(lane < 64, -si, si)
                for h in heads:
                    x = acc[at, h * 128 : (h + 1) * 128]
                    y = (x * co + pltpu.roll(x, 64, 1) * si).astype(jnp.bfloat16)
                    if h < 4:
                        Q[h, at, :] = y
                    else:
                        KV[c, 0, at, :] = y
                        KV[c, 1, at, :] = acc[at, 640:768].astype(jnp.bfloat16)
                return carry

            lax.fori_loop(0, 256 // step, rope, 0)

    rotate((4,))
    @pl.when(turn == 1)
    def _():
        along(0, low, 1).wait_recv()
        along(2, low, 1).start()

    @pl.when(turn == 3)
    def _():
        along(1, high, -1).wait_recv()
        along(3, high, -1).start()

    kv0 = net.send(KV.at[c], m.P)
    kv1 = {s: net.send(KV.at[c], m.Z[s]) for s in SIDES}

    wo0 = {s: net.plan(strip(m.xl, d, s), m.P) for s in SIDES}

    @pl.when(turn == 0)
    def _():
        for s in SIDES:
            net.start(wo0[s])

    acc[:, pl.ds(0, 256)] = columns((m.z, m.zo[1], m.zo[-1], m.z2), 0)

    acc[:, pl.ds(256, 256)] = columns((m.z, m.zo[1], m.zo[-1], m.z2), 256)

    @pl.when(turn == 1)
    def _():
        along(4, high, 1).wait_recv()

    @pl.when(turn == 3)
    def _():
        along(5, low, -1).wait_recv()

    @pl.when(turn % 2 == 1)
    def _():
        for s in SIDES:
            net.start(wo1[s])
        for s in SIDES:
            net.start(wo0[s])

    rotate((0, 1, 2, 3))

    def bias(s, ctx, half):
        return jnp.where(order[2 * ctx + half] < order[2 * c + s], 0.0, NEG).astype(jnp.float32)

    ones = jnp.ones((512, 128), jnp.bfloat16)
    row = lax.broadcasted_iota(jnp.int32, (256, 256), 0)
    col = lax.broadcasted_iota(jnp.int32, (256, 256), 1)

    def tile(h, s, at, size, ctxs, first, lift):
        q = Q[h, at, :]
        pieces = []
        for ctx, lift_ in zip(ctxs, lift):
            x = lax.dot_general(q, KV[ctx, 0], (((1,), (1,)), ((), ())), preferred_element_type=jnp.float32)
            for half in range(2):
                y = x[:, half * 256 : (half + 1) * 256]
                if first and half == s:
                    y = jnp.where(row >= col, y, NEG)
                pieces.append((y, lift_[s][half]))
        top = None
        for y, b in pieces:
            e = jnp.maximum(y[:, :128], y[:, 128:]) + b
            top = e if top is None else jnp.maximum(top, e)
        new = jnp.broadcast_to(jnp.max(top, axis=1, keepdims=True), (size, 128))
        if not first:
            old = peak[h, at, :]
            new = jnp.maximum(old, new)
        level = new * SCALE
        p = []
        for y, b in pieces:
            down = b - level
            p.append(jnp.exp2(y * SCALE + jnp.concatenate([down, down], axis=1)).astype(jnp.bfloat16))
        part = None
        for i, ctx in enumerate(ctxs):
            value = jnp.concatenate([KV[ctx, 1], ones], axis=1)
            one = jnp.dot(jnp.concatenate(p[2 * i : 2 * i + 2], axis=1), value, preferred_element_type=jnp.float32)
            part = one if part is None else part + one
        if not first:
            factor = jnp.exp2((old - new) * SCALE)
            part = num[h, at, :] * jnp.concatenate([factor, factor], axis=1) + part
        return new, part

    def lifts(ctxs, first=False):
        out = []
        for ctx in ctxs:
            out.append([[jnp.float32(0.0) if first and s == half else bias(s, ctx, half) for half in range(2)] for s in range(2)])
        return out

    def tiles(h, ctxs, first, lift):
        size = 128 if len(ctxs) > 1 else 256
        out = []
        for s in range(2):
            for at in range(s * 256, (s + 1) * 256, size):
                at = pl.ds(at, size)
                out.append((at, tile(h, s, at, size, ctxs, first, lift)))
        return out

    def attend(ctxs, first=False, between=None):
        lift = lifts(ctxs, first)
        for h in range(4):
            if between is not None and h == 2:
                between()
            for at, (new, part) in tiles(h, ctxs, first, lift):
                peak[h, at, :], num[h, at, :] = new, part

    kv2, kv3, kv4, wo2, wo3, wo4 = {}, {}, {}, {}, {}, {}
    part_of = {1: 0, -1: 1}
    def to_z():
        net.recv(kv0, KV.at[m.c1])
        for s in SIDES:
            kv2[s] = net.send(KV.at[m.c1], m.Z[s])

        @pl.when(turn == 2)
        def _():
            along(2, low, 1).wait_recv()
            along(3, high, -1).wait_recv()
            for s in SIDES:
                net.start(wo1[s])
            for s in SIDES:
                net.start(wo0[s])

    attend((c,), True, to_z)

    for s in SIDES:
        there = 2 * m.zo[s] + m.xl
        net.recv(kv1[s], KV.at[there])
        kv3[s] = net.send(KV.at[there, part_of[s]], m.Z[s])
    attend([2 * m.zo[s] + m.xl for s in SIDES])
    for s in SIDES:
        wo3[s] = net.plan(strip(m.xl, m.yo[s], s), m.Y[s])

    def pass_on():
        for s in SIDES:
            net.recv(wo1[s], strip(m.xl, m.yo[s]))
            net.start(wo3[s])

    @pl.when(turn == 0)
    def _():
        pass_on()

    attend((m.c1,))
    for s in SIDES:
        there = 2 * m.zo[s] + m.xo
        net.recv(kv2[s], KV.at[there])
        kv4[s] = net.send(KV.at[there, part_of[s]], m.Z[s])
    for s in SIDES:
        net.recv(kv3[s], KV.at[2 * m.z2 + m.xl, part_of[s]])
    for r in SIDES:
        for s in SIDES:
            wo2[r, s] = net.plan(strip(m.xo, d, r), m.Y[s])

    def cross():
        for r in SIDES:
            net.recv(wo0[r], strip(m.xo, d, r))
            for s in SIDES:
                net.start(wo2[r, s])

    @pl.when(turn % 2 == 1)
    def _():
        pass_on()

    attend((2 * m.z2 + m.xl,))

    @pl.when(turn != 2)
    def _():
        cross()

    attend([2 * m.zo[s] + m.xo for s in SIDES])

    @pl.when(turn == 2)
    def _():
        pass_on()
        cross()


    for s in SIDES:
        net.recv(kv4[s], KV.at[2 * m.z2 + m.xo, part_of[s]])

    last = (2 * m.z2 + m.xo,)
    lift = lifts(last)
    top, bottom = pl.ds(0, 256), pl.ds(256, 256)
    kA = []
    for h in range(4):
        for at, (_, part) in tiles(h, last, False, lift):
            AT[t, h, at, :] = (part[:, :128] / part[:, 128:]).astype(jnp.bfloat16)
        ks = [net.send(AT.at[t, h, pl.ds(s * 256, 256)], (m.P, m.Q)[s], RA.at[s, h]) for s in range(2)]
        ks.append(net.send(AT.at[t, h], m.C))
        kA.append(ks)
    for s in SIDES:
        wo4[s] = net.plan(strip(m.xo, m.yo[s], s), m.Y[s])

    def hop(now):
        @pl.when(now)
        def _():
            for s in SIDES:
                net.recv(wo2[s, s], strip(m.xo, m.yo[s], s))
                net.start(wo4[s])

    hop(turn == 0)
    kR = []
    for h in range(4):
        net.recv(kA[h][0], RA.at[0, h])
        a = net.send(RA.at[0, h], m.Q, AT.at[t, h, top])
        net.recv(kA[h][1], RA.at[1, h])
        kR.append((a, net.send(RA.at[1, h], m.P, AT.at[m.t2, h, bottom])))
        if h == 1:
            hop(turn % 2 == 1)
    soon = [[(m.xl, d), (m.xl, m.yo[1])], [(m.xl, m.yo[-1]), (m.xl, m.y2)], [(m.xo, d), (m.xo, m.yo[1])]]
    last_two = [(m.xo, m.yo[-1]), (m.xo, m.y2)]

    def product(bs, two):
        left = jnp.concatenate([AT[b, h] for b in bs for h in range(4)], axis=1)
        right = jnp.concatenate(
            [jnp.concatenate([WO[xl * 4 + y, pl.ds(b * 512, 512), :] for b in bs], axis=0) for xl, y in two], axis=1
        )
        return jnp.dot(left, right, preferred_element_type=jnp.float32)

    def project(bs, twos, first=False):
        for two in twos:
            part = product(bs, two)
            for i, (xl, y) in enumerate(two):
                cols = pl.ds(pl.multiple_of((xl * 4 + y) * 128, 128), 128)
                piece = part[:, i * 128 : (i + 1) * 128]
                if first:
                    total[:, cols] = piece
                else:
                    total[:, cols] += piece

    for h in range(4):
        net.recv(kA[h][2], AT.at[m.t1, h])
    project((t, m.t1), soon[:1], True)
    kD = []
    for h in range(4):
        net.recv(kR[h][0], AT.at[m.t2, h, top])
        net.recv(kR[h][1], AT.at[m.t2, h, bottom])
        kD.append(net.send(AT.at[m.t2, h], m.C))
    hop(turn == 2)

    for s in SIDES:
        net.recv(wo3[s], strip(m.xl, m.y2, s))
    net.recv(wo2[-1, 1], strip(m.xo, m.yo[1], -1))
    net.recv(wo2[1, -1], strip(m.xo, m.yo[-1], 1))
    project((t, m.t1), soon[1:], True)
    project((m.t2,), soon)
    for h in range(4):
        net.recv(kD[h], AT.at[m.t3, h])
    project((m.t3,), soon)
    later.wait()

    def close(two, part):
        for xl, y in two:
            cols = pl.ds(pl.multiple_of((xl * 4 + y) * 128, 128), 128)
            for i in range(4):
                at = pl.ds(i * 128, 128)
                branch = total[at, cols].astype(jnp.bfloat16)
                out[at, cols] = branch
                gap = H[t, at, cols].astype(jnp.float32) + branch.astype(jnp.float32) - T[at, cols].astype(jnp.float32)
                sq = gap * gap
                fold = [sq[r * 8 : (r + 1) * 8] for r in range(16)]
                while len(fold) > 1:
                    fold = [a + b for a, b in zip(fold[::2], fold[1::2])]
                part = part + fold[0]
        return part

    part = jnp.zeros((8, 128), jnp.float32)
    for two in soon:
        part = close(two, part)
    for s in SIDES:
        net.recv(wo4[s], strip(m.xo, m.y2, s))
    rest = product((t, m.t1, m.t2, m.t3), last_two)
    for i, (xl, y) in enumerate(last_two):
        total[:, pl.ds(pl.multiple_of((xl * 4 + y) * 128, 128), 128)] = rest[:, i * 128 : (i + 1) * 128]
    part = close(last_two, part)
    rings = (
        (8, m.xl * 4 + t, lambda i: (2 * m.z + i // 4, i % 4, d)),
        (16, m.z * 4 + d, lambda i: (2 * (i // 4) + m.xl, t, i % 4)),
    )
    for number, (size, me, device) in enumerate(rings):
        LB[number, me] = part
        for j in range(1, size):
            pltpu.make_async_remote_copy(
                src_ref=LB.at[number, me], dst_ref=LB.at[number, me], send_sem=osend.at[5 + number],
                recv_sem=orecv.at[8 + number], device_id=device((me + j) % size), device_id_type=MESH,
            ).start()
        others = LB.at[number, pl.ds(0, size - 1)]
        pltpu.make_async_copy(others, others, orecv.at[8 + number]).wait()
        pltpu.make_async_copy(others, others, osend.at[5 + number]).wait()
        part = LB[number, 0]
        for j in range(1, size):
            part = part + LB[number, j]
    loss_out[0, 0] = jnp.sum(part) / (4 * 4096 * MODEL_WIDTH)
    net.finish()

    @pl.when(t != m.z)
    def _():
        meet(t).wait_send()

    for k, ref, s, when in ((0, low, 1, 0), (1, high, -1, 0), (4, high, 1, 0), (5, low, -1, 0), (2, low, 1, 1), (3, high, -1, 3)):
        @pl.when(turn == when)
        def _(k=k, ref=ref, s=s):
            along(k, ref, s).wait_send()


def tables():
    freqs = ROPE_BASE ** (-(np.arange(64) * 2.0) / HEAD_SIZE)
    freqs = np.concatenate([freqs, freqs])[None, :]
    rows, blocks = np.arange(256)[:, None] * freqs, np.arange(16)[:, None] * 256 * freqs
    return [f(x).astype(np.float32) for x in (rows, blocks) for f in (np.cos, np.sin)]


def on_device(hidden, target, gain, w_query, w_key, value_matrix, w_out, block_order):
    any_spec = pl.BlockSpec(memory_space=pl.ANY)
    vmem = pl.BlockSpec(memory_space=pltpu.VMEM)
    smem = pl.BlockSpec(memory_space=pltpu.SMEM)
    bf16, f32 = jnp.bfloat16, jnp.float32
    branch, loss = pl.pallas_call(
        layer_kernel,
        out_shape=(pltpu.VMEM((512, 1024), bf16), jax.ShapeDtypeStruct((1, 1), f32)),
        in_specs=[any_spec] * 6 + [vmem, smem, any_spec, any_spec, vmem, vmem],
        out_specs=(vmem, smem),
        scratch_shapes=[
            pltpu.VMEM((4, 512, 1024), bf16),
            pltpu.VMEM((4, 512, 1024), bf16),
            pltpu.VMEM((2, 256, 1024), bf16),
            pltpu.VMEM((8, 4, 128, 768), bf16),
            pltpu.VMEM((512, 768), f32),
            pltpu.VMEM((4, 512, 128), bf16),
            pltpu.VMEM((8, 2, 512, 128), bf16),
            pltpu.VMEM((8, 2048, 128), bf16),
            pltpu.VMEM((4, 4, 512, 128), bf16),
            pltpu.VMEM((2, 4, 256, 128), bf16),
            pltpu.VMEM((4, 512, 256), f32),
            pltpu.VMEM((4, 512, 128), f32),
            pltpu.VMEM((512, 1024), bf16),
            pltpu.VMEM((512, 1024), f32),
            pltpu.VMEM((2, 16, 8, 128), f32),
            pltpu.VMEM((256, 128), f32),
            pltpu.VMEM((256, 128), f32),
            pltpu.SemaphoreType.DMA((POOL,)),
            pltpu.SemaphoreType.DMA((COPIES,)),
            pltpu.SemaphoreType.DMA((8,)),
            pltpu.SemaphoreType.DMA((8,)),
            pltpu.SemaphoreType.DMA((10,)),
            pltpu.SemaphoreType.DMA((6,)),
            pltpu.SemaphoreType.DMA((6,)),
        ],
        compiler_params=pltpu.CompilerParams(
            collective_id=0, has_side_effects=True, vmem_limit_bytes=60 * MIB
        ),
        name="layer",
    )(hidden, target, w_query, w_key, value_matrix, w_out, gain[None, :], block_order, *(jnp.asarray(x) for x in tables()))
    return branch[None], loss.reshape(())


def solution(mesh):
    placed = (
        P("dp", "ctx", "tp"), P("dp", "ctx", "tp"), P(), P(("ctx", "dp"), "tp"), P(("ctx", "dp"), "tp"),
        P(("ctx", "dp"), "tp"), P("tp", ("ctx", "dp")), P(),
    )
    return jax.shard_map(
        on_device, mesh=mesh, in_specs=placed, out_specs=(P("dp", "ctx", "tp"), P()), check_vma=False
    )
```

```python
import types

import jax
import jax.numpy as jnp
import numpy as np
from jax import lax
from jax.experimental import pallas as pl
from jax.experimental.pallas import tpu as pltpu
from jax.sharding import PartitionSpec as P

MODEL_WIDTH = 4096
HEAD_SIZE = 128
ROPE_BASE = 500000.0
NEG = -1e30
SCALE = float(np.log2(np.e) / np.sqrt(HEAD_SIZE))
MIB = 1024 * 1024
POOL = 64
COPIES = 112

MESH = pl.DeviceIdType.MESH
SIDES = (1, -1)


def here():
    c, t, d = lax.axis_index("ctx"), lax.axis_index("tp"), lax.axis_index("dp")
    return c, t, d


class Net:
    def __init__(self, send_sems, recv_sems):
        self.send_sems, self.recv_sems = send_sems, recv_sems
        self.started = []

    def copy(self, k, src, dst, dev):
        c, t, d = dev
        return pltpu.make_async_remote_copy(
            src_ref=src,
            dst_ref=dst,
            send_sem=self.send_sems.at[k % POOL],
            recv_sem=self.recv_sems.at[k],
            device_id=(c, t, d),
            device_id_type=MESH,
        )

    def plan(self, ref, dev, dst=None):
        k = len(self.started)
        if k >= POOL:
            self.started[k - POOL][0].wait_send()
        self.started.append((self.copy(k, ref, ref if dst is None else dst, dev), dev))
        return k

    def start(self, k):
        self.started[k][0].start()

    def send(self, ref, dev, dst=None):
        k = self.plan(ref, dev, dst)
        self.start(k)
        return k

    def recv(self, k, ref):
        self.copy(k, ref, ref, self.started[k][1]).wait_recv()

    def finish(self):
        assert len(self.started) <= COPIES
        for copy, _ in self.started[-POOL:]:
            copy.wait_send()


def places():
    c, t, d = here()
    z, xl = c // 2, c % 2
    c1 = c + 1 - 2 * xl
    t1 = t + 1 - 2 * (t % 2)
    t2 = (t + 2) % 4
    t3 = (t1 + 2) % 4
    return types.SimpleNamespace(
        c=c, t=t, d=d, z=z, xl=xl, xo=1 - xl, c1=c1, t1=t1, t2=t2, t3=t3,
        P=(c1, t, d), Q=(c1, t2, d), C=(c, t1, d), R=(c, t2, d), D=(c, t3, d),
        Y={s: (c, t, (d + s) % 4) for s in SIDES},
        Z={s: ((c + 2 * s) % 8, t, d) for s in SIDES},
        yo={s: (d - s) % 4 for s in SIDES},
        zo={s: (z - s) % 4 for s in SIDES},
        y2=(d + 2) % 4, z2=(z + 2) % 4,
    )


def greet(m):
    barrier = pltpu.get_barrier_semaphore()
    others = [m.P, m.Q, m.C, m.R, m.D, m.Y[1], m.Y[-1], m.Z[1], m.Z[-1]]
    for dev in others:
        pl.semaphore_signal(barrier, inc=1, device_id=dev, device_id_type=MESH)
    pl.semaphore_wait(barrier, len(others))


def layer_kernel(
    hid, tgt, wq, wk, wv, wo, gain, order, turn_cos, turn_sin, block_cos, block_sin,
    out, loss_out,
    H, N, RH, W, acc, Q, KV, WO, AT, RA, num, peak, T, total, LB, row_cos, row_sin, ssem, rsem, lsem, osend, orecv, zsend, zrecv,
):
    m = places()
    net = Net(ssem, rsem)
    c, t, d = m.c, m.t, m.d
    local = [
        pltpu.make_async_copy(wq, W.at[c, d, :, pl.ds(0, 512)], lsem.at[0]),
        pltpu.make_async_copy(wk, W.at[c, d, :, pl.ds(512, 128)], lsem.at[1]),
        pltpu.make_async_copy(wv, W.at[c, d, :, pl.ds(640, 128)], lsem.at[2]),
        pltpu.make_async_copy(hid.at[0], H.at[t], lsem.at[3]),
    ]
    for cp in local:
        cp.start()
    later = pltpu.make_async_copy(tgt.at[0], T, lsem.at[4])
    later.start()
    turns = [
        pltpu.make_async_copy(turn_cos, row_cos, lsem.at[6]),
        pltpu.make_async_copy(turn_sin, row_sin, lsem.at[7]),
    ]
    for cp in turns:
        cp.start()
    own_wo = pltpu.make_async_copy(wo, WO.at[m.xl * 4 + d, pl.ds(m.z * 512, 512)], lsem.at[5])
    greet(m)
    for cp in local:
        cp.wait()

    def pair(z):
        return pl.ds(2 * z, 2)

    qa = {1: pl.ds(0, 32), -1: pl.ds(32, 32)}
    qb = {1: pl.ds(64, 32), -1: pl.ds(96, 32)}
    ha, hb = pl.ds(0, 64), pl.ds(64, 64)
    parts = 4
    rows = 256 // parts

    kX = net.send(W.at[c, d], m.P)
    kY1 = {s: net.send(W.at[c, d], m.Y[s]) for s in SIDES}
    kZ1 = {s: net.send(W.at[c, d], m.Z[s]) for s in SIDES}
    kH0 = [net.send(H.at[t, pl.ds(i * rows, rows)], m.P, RH.at[0, pl.ds(i * rows, rows)]) for i in range(parts)]
    kH1 = [net.send(H.at[t, pl.ds(256 + i * rows, rows)], m.Q, RH.at[1, pl.ds(i * rows, rows)]) for i in range(parts)]
    kC = net.send(H.at[t], m.C)

    mine = WO.at[m.xl * 4 + d]
    block = WO.at[m.xl * 4 + d, pl.ds(t * 512, 512)]

    def meet(k):
        return pltpu.make_async_remote_copy(
            src_ref=wo, dst_ref=block, send_sem=osend.at[4], recv_sem=orecv.at[4 + k],
            device_id=(c, m.z, d), device_id_type=MESH,
        )

    @pl.when(t == m.z)
    def _():
        own_wo.start()

    @pl.when(t != m.z)
    def _():
        meet(t).start()

    net.recv(kX, W.at[m.c1, d])
    kY2 = {s: net.send(W.at[m.c1, d], m.Y[s]) for s in SIDES}
    kZ2 = {s: net.send(W.at[m.c1, d], m.Z[s]) for s in SIDES}

    def relay(i):
        net.recv(kH0[i], RH.at[0, pl.ds(i * rows, rows)])
        a = net.send(RH.at[0, pl.ds(i * rows, rows)], m.Q, H.at[t, pl.ds(i * rows, rows)])
        net.recv(kH1[i], RH.at[1, pl.ds(i * rows, rows)])
        b = net.send(RH.at[1, pl.ds(i * rows, rows)], m.P, H.at[m.t2, pl.ds(256 + i * rows, rows)])
        return a, b

    far = []

    def landed(i):
        for k_, lo in ((kF[i][0], i * rows), (kF[i][1], 256 + i * rows)):
            net.recv(k_, H.at[m.t2, pl.ds(lo, rows)])
            far.append((net.send(H.at[m.t2, pl.ds(lo, rows)], m.C), lo))

    kF = []
    fY, fZ, kY3, kZ3, kY4, kZ4 = {}, {}, {}, {}, {}, {}
    for s in SIDES:
        net.recv(kY1[s], W.at[c, m.yo[s]])
        net.recv(kZ1[s], W.at[2 * m.zo[s] + m.xl, d])
    kF.append(relay(0))
    for s in SIDES:
        net.recv(kY2[s], W.at[m.c1, m.yo[s]])
        kY3[s] = net.send(W.at[pair(m.z), m.yo[s], qa[s]], m.Y[s])
        net.recv(kZ2[s], W.at[2 * m.zo[s] + m.xo, d])
        kZ3[s] = net.send(W.at[pair(m.zo[s]), d, qb[s]], m.Z[s])
    for s in SIDES:
        for r in SIDES:
            kZ4[s, r] = net.send(W.at[pair(m.z), m.yo[s], ha], m.Z[r])
            kY4[s, r] = net.send(W.at[pair(m.zo[s]), d, hb], m.Y[r])

    kF += [relay(1), relay(2)]
    kY6, kZ6 = {}, {}
    for s in SIDES:
        net.recv(kY3[s], W.at[pair(m.z), m.y2, qa[s]])
        net.recv(kZ3[s], W.at[pair(m.z2), d, qb[s]])
    for r in SIDES:
        kZ6[r] = net.send(W.at[pair(m.z), m.y2, ha], m.Z[r])
        kY6[r] = net.send(W.at[pair(m.z2), d, hb], m.Y[r])
    for s in SIDES:
        fZ[s, "own"] = net.send(W.at[pair(m.zo[s]), d, qa[s]], m.Z[s])
        fY[s, "own"] = net.send(W.at[pair(m.z), m.yo[s], qb[s]], m.Y[s])
    kF.append(relay(3))
    for s in SIDES:
        for r in SIDES:
            net.recv(kZ4[s, r], W.at[pair(m.zo[r]), m.yo[s], ha])
            fZ[r, s] = net.send(W.at[pair(m.zo[r]), m.yo[s], qa[r]], m.Z[r])
            net.recv(kY4[s, r], W.at[pair(m.zo[s]), m.yo[r], hb])
            fY[r, s] = net.send(W.at[pair(m.zo[s]), m.yo[r], qb[r]], m.Y[r])
    landed(0)
    landed(1)
    landed(2)
    landed(3)
    for r in SIDES:
        net.recv(kZ6[r], W.at[pair(m.zo[r]), m.y2, ha])
        fZ[r, "far"] = net.send(W.at[pair(m.zo[r]), m.y2, qa[r]], m.Z[r])
        net.recv(kY6[r], W.at[pair(m.z2), m.yo[r], hb])
        fY[r, "far"] = net.send(W.at[pair(m.z2), m.yo[r], qb[r]], m.Y[r])
    turn = (m.z - t + 4) % 4

    def along(k, ref, s):
        return pltpu.make_async_remote_copy(
            src_ref=ref, dst_ref=ref, send_sem=zsend.at[k], recv_sem=zrecv.at[k],
            device_id=m.Z[s], device_id_type=MESH,
        )

    low = WO.at[m.xl * 4 + d, pl.ds(0, 1024)]
    high = WO.at[m.xl * 4 + d, pl.ds(1024, 1024)]

    @pl.when(turn == 0)
    def _():
        own_wo.wait()
        for k in range(4):
            @pl.when(k != t)
            def _(k=k):
                there = WO.at[m.xl * 4 + d, pl.ds(k * 512, 512)]
                pltpu.make_async_remote_copy(
                    src_ref=there, dst_ref=there, send_sem=osend.at[4], recv_sem=orecv.at[4 + k],
                    device_id=(c, m.z, d), device_id_type=MESH,
                ).wait_recv()

        along(0, low, 1).start()
        along(1, high, -1).start()
        along(4, high, 1).start()
        along(5, low, -1).start()

    def strip(xl, y, s=None):
        return WO.at[xl * 4 + y] if s is None else WO.at[xl * 4 + y, pl.ds(0 if s == 1 else 1024, 1024)]

    wo1 = {s: net.plan(mine, m.Y[s]) for s in SIDES}

    @pl.when(turn == 0)
    def _():
        for s in SIDES:
            net.start(wo1[s])

    net.recv(kC, H.at[m.t1])
    for k, lo in far:
        net.recv(k, H.at[m.t3, pl.ds(lo, rows)])


    step = 64

    def norm(i, carry):
        at = pl.ds(pl.multiple_of(i * step, step), step)
        total = jnp.zeros((step, 1), jnp.float32)
        for b in range(4):
            x = H[b, at, :].astype(jnp.float32)
            total = total + jnp.sum(x * x, axis=1, keepdims=True)
        scale = lax.rsqrt(total * (1.0 / MODEL_WIDTH) + 1e-05)
        for b in range(4):
            x = H[b, at, :].astype(jnp.float32)
            g = gain[:, b * 1024 : (b + 1) * 1024]
            N[b, at, :] = (x * scale * g).astype(jnp.bfloat16)
        return carry

    lax.fori_loop(0, 512 // step, norm, 0)

    def columns(zs, lo):
        cols = pl.ds(lo, 256)
        sums = None
        for z in zs:
            w = W[pair(z), :, :, cols].reshape(1024, 256)
            part = jnp.dot(N[z], w, preferred_element_type=jnp.float32)
            sums = part if sums is None else sums + part
        return sums

    for r in SIDES:
        net.recv(fY[r, "own"], W.at[pair(m.z), m.y2, qb[r]])
        for s in SIDES:
            net.recv(fY[r, s], W.at[pair(m.zo[s]), m.y2, qb[r]])
    acc[:, pl.ds(512, 256)] = columns((m.z, m.zo[1], m.zo[-1]), 512)

    for r in SIDES:
        net.recv(fZ[r, "own"], W.at[pair(m.z2), d, qa[r]])
        for s in SIDES:
            net.recv(fZ[r, s], W.at[pair(m.z2), m.yo[s], qa[r]])
        net.recv(fZ[r, "far"], W.at[pair(m.z2), m.y2, qa[r]])
        net.recv(fY[r, "far"], W.at[pair(m.z2), m.y2, qb[r]])
    acc[:, pl.ds(512, 256)] += columns((m.z2,), 512)
    for cp in turns:
        cp.wait()

    def rotate(heads):
        for s in range(2):
            where = order[2 * c + s]
            bc, bs = block_cos[pl.ds(where, 1), :], block_sin[pl.ds(where, 1), :]

            def rope(i, carry, s=s, bc=bc, bs=bs):
                rows_at = pl.ds(pl.multiple_of(i * step, step), step)
                at = pl.ds(pl.multiple_of(s * 256 + i * step, step), step)
                rc, rs = row_cos[rows_at, :], row_sin[rows_at, :]
                co = rc * bc - rs * bs
                si = rs * bc + rc * bs
                lane = lax.broadcasted_iota(jnp.int32, (step, 128), 1)
                si = jnp.where(lane < 64, -si, si)
                for h in heads:
                    x = acc[at, h * 128 : (h + 1) * 128]
                    y = (x * co + pltpu.roll(x, 64, 1) * si).astype(jnp.bfloat16)
                    if h < 4:
                        Q[h, at, :] = y
                    else:
                        KV[c, 0, at, :] = y
                        KV[c, 1, at, :] = acc[at, 640:768].astype(jnp.bfloat16)
                return carry

            lax.fori_loop(0, 256 // step, rope, 0)

    rotate((4,))
    @pl.when(turn == 1)
    def _():
        along(0, low, 1).wait_recv()
        along(2, low, 1).start()

    @pl.when(turn == 3)
    def _():
        along(1, high, -1).wait_recv()
        along(3, high, -1).start()

    kv0 = net.send(KV.at[c], m.P)
    kv1 = {s: net.send(KV.at[c], m.Z[s]) for s in SIDES}

    wo0 = {s: net.plan(strip(m.xl, d, s), m.P) for s in SIDES}

    @pl.when(turn == 0)
    def _():
        for s in SIDES:
            net.start(wo0[s])

    acc[:, pl.ds(0, 256)] = columns((m.z, m.zo[1], m.zo[-1], m.z2), 0)

    acc[:, pl.ds(256, 256)] = columns((m.z, m.zo[1], m.zo[-1], m.z2), 256)

    @pl.when(turn == 1)
    def _():
        along(4, high, 1).wait_recv()

    @pl.when(turn == 3)
    def _():
        along(5, low, -1).wait_recv()

    @pl.when(turn % 2 == 1)
    def _():
        for s in SIDES:
            net.start(wo1[s])
        for s in SIDES:
            net.start(wo0[s])

    rotate((0, 1, 2, 3))

    def bias(s, ctx, half):
        return jnp.where(order[2 * ctx + half] < order[2 * c + s], 0.0, NEG).astype(jnp.float32)

    ones = jnp.ones((512, 128), jnp.bfloat16)
    row = lax.broadcasted_iota(jnp.int32, (256, 256), 0)
    col = lax.broadcasted_iota(jnp.int32, (256, 256), 1)

    def tile(h, s, at, size, ctxs, first, lift):
        q = Q[h, at, :]
        pieces = []
        for ctx, lift_ in zip(ctxs, lift):
            x = lax.dot_general(q, KV[ctx, 0], (((1,), (1,)), ((), ())), preferred_element_type=jnp.float32)
            for half in range(2):
                y = x[:, half * 256 : (half + 1) * 256]
                if first and half == s:
                    y = jnp.where(row >= col, y, NEG)
                pieces.append((y, lift_[s][half]))
        top = None
        for y, b in pieces:
            e = jnp.maximum(y[:, :128], y[:, 128:]) + b
            top = e if top is None else jnp.maximum(top, e)
        new = jnp.broadcast_to(jnp.max(top, axis=1, keepdims=True), (size, 128))
        if not first:
            old = peak[h, at, :]
            new = jnp.maximum(old, new)
        level = new * SCALE
        p = []
        for y, b in pieces:
            down = b - level
            p.append(jnp.exp2(y * SCALE + jnp.concatenate([down, down], axis=1)).astype(jnp.bfloat16))
        part = None
        for i, ctx in enumerate(ctxs):
            value = jnp.concatenate([KV[ctx, 1], ones], axis=1)
            one = jnp.dot(jnp.concatenate(p[2 * i : 2 * i + 2], axis=1), value, preferred_element_type=jnp.float32)
            part = one if part is None else part + one
        if not first:
            factor = jnp.exp2((old - new) * SCALE)
            part = num[h, at, :] * jnp.concatenate([factor, factor], axis=1) + part
        return new, part

    def lifts(ctxs, first=False):
        out = []
        for ctx in ctxs:
            out.append([[jnp.float32(0.0) if first and s == half else bias(s, ctx, half) for half in range(2)] for s in range(2)])
        return out

    def tiles(h, ctxs, first, lift):
        size = 128 if len(ctxs) > 1 else 256
        out = []
        for s in range(2):
            for at in range(s * 256, (s + 1) * 256, size):
                at = pl.ds(at, size)
                out.append((at, tile(h, s, at, size, ctxs, first, lift)))
        return out

    def attend(ctxs, first=False, between=None):
        lift = lifts(ctxs, first)
        for h in range(4):
            if between is not None and h == 2:
                between()
            for at, (new, part) in tiles(h, ctxs, first, lift):
                peak[h, at, :], num[h, at, :] = new, part

    kv2, kv3, kv4, wo2, wo3, wo4 = {}, {}, {}, {}, {}, {}
    part_of = {1: 0, -1: 1}
    def to_z():
        net.recv(kv0, KV.at[m.c1])
        for s in SIDES:
            kv2[s] = net.send(KV.at[m.c1], m.Z[s])

        @pl.when(turn == 2)
        def _():
            along(2, low, 1).wait_recv()
            along(3, high, -1).wait_recv()
            for s in SIDES:
                net.start(wo1[s])
            for s in SIDES:
                net.start(wo0[s])

    attend((c,), True, to_z)

    for s in SIDES:
        there = 2 * m.zo[s] + m.xl
        net.recv(kv1[s], KV.at[there])
        kv3[s] = net.send(KV.at[there, part_of[s]], m.Z[s])
    attend([2 * m.zo[s] + m.xl for s in SIDES])
    for s in SIDES:
        wo3[s] = net.plan(strip(m.xl, m.yo[s], s), m.Y[s])

    def pass_on():
        for s in SIDES:
            net.recv(wo1[s], strip(m.xl, m.yo[s]))
            net.start(wo3[s])

    @pl.when(turn == 0)
    def _():
        pass_on()

    attend((m.c1,))
    for s in SIDES:
        there = 2 * m.zo[s] + m.xo
        net.recv(kv2[s], KV.at[there])
        kv4[s] = net.send(KV.at[there, part_of[s]], m.Z[s])
    for s in SIDES:
        net.recv(kv3[s], KV.at[2 * m.z2 + m.xl, part_of[s]])
    for r in SIDES:
        for s in SIDES:
            wo2[r, s] = net.plan(strip(m.xo, d, r), m.Y[s])

    def cross():
        for r in SIDES:
            net.recv(wo0[r], strip(m.xo, d, r))
            for s in SIDES:
                net.start(wo2[r, s])

    @pl.when(turn % 2 == 1)
    def _():
        pass_on()

    attend((2 * m.z2 + m.xl,))

    @pl.when(turn != 2)
    def _():
        cross()

    attend([2 * m.zo[s] + m.xo for s in SIDES])

    @pl.when(turn == 2)
    def _():
        pass_on()
        cross()


    for s in SIDES:
        net.recv(kv4[s], KV.at[2 * m.z2 + m.xo, part_of[s]])

    last = (2 * m.z2 + m.xo,)
    lift = lifts(last)
    top, bottom = pl.ds(0, 256), pl.ds(256, 256)
    kA = []
    for h in range(4):
        for at, (_, part) in tiles(h, last, False, lift):
            AT[t, h, at, :] = (part[:, :128] / part[:, 128:]).astype(jnp.bfloat16)
        ks = [net.send(AT.at[t, h, pl.ds(s * 256, 256)], (m.P, m.Q)[s], RA.at[s, h]) for s in range(2)]
        ks.append(net.send(AT.at[t, h], m.C))
        kA.append(ks)
    for s in SIDES:
        wo4[s] = net.plan(strip(m.xo, m.yo[s], s), m.Y[s])

    def hop(now):
        @pl.when(now)
        def _():
            for s in SIDES:
                net.recv(wo2[s, s], strip(m.xo, m.yo[s], s))
                net.start(wo4[s])

    hop(turn == 0)
    kR = []
    for h in range(4):
        net.recv(kA[h][0], RA.at[0, h])
        a = net.send(RA.at[0, h], m.Q, AT.at[t, h, top])
        net.recv(kA[h][1], RA.at[1, h])
        kR.append((a, net.send(RA.at[1, h], m.P, AT.at[m.t2, h, bottom])))
    soon = [[(m.xl, d), (m.xl, m.yo[1])], [(m.xl, m.yo[-1]), (m.xl, m.y2)], [(m.xo, d), (m.xo, m.yo[1])]]
    last_two = [(m.xo, m.yo[-1]), (m.xo, m.y2)]

    def product(bs, two):
        left = jnp.concatenate([AT[b, h] for b in bs for h in range(4)], axis=1)
        right = jnp.concatenate(
            [jnp.concatenate([WO[xl * 4 + y, pl.ds(b * 512, 512), :] for b in bs], axis=0) for xl, y in two], axis=1
        )
        return jnp.dot(left, right, preferred_element_type=jnp.float32)

    def project(bs, twos, first=False):
        for two in twos:
            part = product(bs, two)
            for i, (xl, y) in enumerate(two):
                cols = pl.ds(pl.multiple_of((xl * 4 + y) * 128, 128), 128)
                piece = part[:, i * 128 : (i + 1) * 128]
                if first:
                    total[:, cols] = piece
                else:
                    total[:, cols] += piece

    for h in range(4):
        net.recv(kA[h][2], AT.at[m.t1, h])
    project((t, m.t1), soon[:1], True)
    kD = []
    for h in range(4):
        net.recv(kR[h][0], AT.at[m.t2, h, top])
        net.recv(kR[h][1], AT.at[m.t2, h, bottom])
        kD.append(net.send(AT.at[m.t2, h], m.C))
        if h == 1:
            hop(turn % 2 == 1)
    hop(turn == 2)

    for s in SIDES:
        net.recv(wo3[s], strip(m.xl, m.y2, s))
    net.recv(wo2[-1, 1], strip(m.xo, m.yo[1], -1))
    net.recv(wo2[1, -1], strip(m.xo, m.yo[-1], 1))
    project((t, m.t1), soon[1:], True)
    project((m.t2,), soon)
    for h in range(4):
        net.recv(kD[h], AT.at[m.t3, h])
    project((m.t3,), soon)
    later.wait()

    def close(two, part):
        for xl, y in two:
            cols = pl.ds(pl.multiple_of((xl * 4 + y) * 128, 128), 128)
            for i in range(4):
                at = pl.ds(i * 128, 128)
                branch = total[at, cols].astype(jnp.bfloat16)
                out[at, cols] = branch
                gap = H[t, at, cols].astype(jnp.float32) + branch.astype(jnp.float32) - T[at, cols].astype(jnp.float32)
                sq = gap * gap
                fold = [sq[r * 8 : (r + 1) * 8] for r in range(16)]
                while len(fold) > 1:
                    fold = [a + b for a, b in zip(fold[::2], fold[1::2])]
                part = part + fold[0]
        return part

    part = jnp.zeros((8, 128), jnp.float32)
    for two in soon:
        part = close(two, part)
    for s in SIDES:
        net.recv(wo4[s], strip(m.xo, m.y2, s))
    rest = product((t, m.t1, m.t2, m.t3), last_two)
    for i, (xl, y) in enumerate(last_two):
        total[:, pl.ds(pl.multiple_of((xl * 4 + y) * 128, 128), 128)] = rest[:, i * 128 : (i + 1) * 128]
    part = close(last_two, part)
    rings = (
        (8, m.xl * 4 + t, lambda i: (2 * m.z + i // 4, i % 4, d)),
        (16, m.z * 4 + d, lambda i: (2 * (i // 4) + m.xl, t, i % 4)),
    )
    for number, (size, me, device) in enumerate(rings):
        LB[number, me] = part
        for j in range(1, size):
            pltpu.make_async_remote_copy(
                src_ref=LB.at[number, me], dst_ref=LB.at[number, me], send_sem=osend.at[5 + number],
                recv_sem=orecv.at[8 + number], device_id=device((me + j) % size), device_id_type=MESH,
            ).start()
        others = LB.at[number, pl.ds(0, size - 1)]
        pltpu.make_async_copy(others, others, orecv.at[8 + number]).wait()
        pltpu.make_async_copy(others, others, osend.at[5 + number]).wait()
        part = LB[number, 0]
        for j in range(1, size):
            part = part + LB[number, j]
    loss_out[0, 0] = jnp.sum(part) / (4 * 4096 * MODEL_WIDTH)
    net.finish()

    @pl.when(t != m.z)
    def _():
        meet(t).wait_send()

    for k, ref, s, when in ((0, low, 1, 0), (1, high, -1, 0), (4, high, 1, 0), (5, low, -1, 0), (2, low, 1, 1), (3, high, -1, 3)):
        @pl.when(turn == when)
        def _(k=k, ref=ref, s=s):
            along(k, ref, s).wait_send()


def tables():
    freqs = ROPE_BASE ** (-(np.arange(64) * 2.0) / HEAD_SIZE)
    freqs = np.concatenate([freqs, freqs])[None, :]
    rows, blocks = np.arange(256)[:, None] * freqs, np.arange(16)[:, None] * 256 * freqs
    return [f(x).astype(np.float32) for x in (rows, blocks) for f in (np.cos, np.sin)]


def on_device(hidden, target, gain, w_query, w_key, value_matrix, w_out, block_order):
    any_spec = pl.BlockSpec(memory_space=pl.ANY)
    vmem = pl.BlockSpec(memory_space=pltpu.VMEM)
    smem = pl.BlockSpec(memory_space=pltpu.SMEM)
    bf16, f32 = jnp.bfloat16, jnp.float32
    branch, loss = pl.pallas_call(
        layer_kernel,
        out_shape=(pltpu.VMEM((512, 1024), bf16), jax.ShapeDtypeStruct((1, 1), f32)),
        in_specs=[any_spec] * 6 + [vmem, smem, any_spec, any_spec, vmem, vmem],
        out_specs=(vmem, smem),
        scratch_shapes=[
            pltpu.VMEM((4, 512, 1024), bf16),
            pltpu.VMEM((4, 512, 1024), bf16),
            pltpu.VMEM((2, 256, 1024), bf16),
            pltpu.VMEM((8, 4, 128, 768), bf16),
            pltpu.VMEM((512, 768), f32),
            pltpu.VMEM((4, 512, 128), bf16),
            pltpu.VMEM((8, 2, 512, 128), bf16),
            pltpu.VMEM((8, 2048, 128), bf16),
            pltpu.VMEM((4, 4, 512, 128), bf16),
            pltpu.VMEM((2, 4, 256, 128), bf16),
            pltpu.VMEM((4, 512, 256), f32),
            pltpu.VMEM((4, 512, 128), f32),
            pltpu.VMEM((512, 1024), bf16),
            pltpu.VMEM((512, 1024), f32),
            pltpu.VMEM((2, 16, 8, 128), f32),
            pltpu.VMEM((256, 128), f32),
            pltpu.VMEM((256, 128), f32),
            pltpu.SemaphoreType.DMA((POOL,)),
            pltpu.SemaphoreType.DMA((COPIES,)),
            pltpu.SemaphoreType.DMA((8,)),
            pltpu.SemaphoreType.DMA((8,)),
            pltpu.SemaphoreType.DMA((10,)),
            pltpu.SemaphoreType.DMA((6,)),
            pltpu.SemaphoreType.DMA((6,)),
        ],
        compiler_params=pltpu.CompilerParams(
            collective_id=0, has_side_effects=True, vmem_limit_bytes=60 * MIB
        ),
        name="layer",
    )(hidden, target, w_query, w_key, value_matrix, w_out, gain[None, :], block_order, *(jnp.asarray(x) for x in tables()))
    return branch[None], loss.reshape(())


def solution(mesh):
    placed = (
        P("dp", "ctx", "tp"), P("dp", "ctx", "tp"), P(), P(("ctx", "dp"), "tp"), P(("ctx", "dp"), "tp"),
        P(("ctx", "dp"), "tp"), P("tp", ("ctx", "dp")), P(),
    )
    return jax.shard_map(
        on_device, mesh=mesh, in_specs=placed, out_specs=(P("dp", "ctx", "tp"), P()), check_vma=False
    )
```

```python
import types

import jax
import jax.numpy as jnp
import numpy as np
from jax import lax
from jax.experimental import pallas as pl
from jax.experimental.pallas import tpu as pltpu
from jax.sharding import PartitionSpec as P

MODEL_WIDTH = 4096
HEAD_SIZE = 128
ROPE_BASE = 500000.0
NEG = -1e30
SCALE = float(np.log2(np.e) / np.sqrt(HEAD_SIZE))
MIB = 1024 * 1024
POOL = 64
COPIES = 118

MESH = pl.DeviceIdType.MESH
SIDES = (1, -1)


def here():
    c, t, d = lax.axis_index("ctx"), lax.axis_index("tp"), lax.axis_index("dp")
    return c, t, d


class Net:
    def __init__(self, send_sems, recv_sems):
        self.send_sems, self.recv_sems = send_sems, recv_sems
        self.started = []

    def copy(self, k, src, dst, dev):
        c, t, d = dev
        return pltpu.make_async_remote_copy(
            src_ref=src,
            dst_ref=dst,
            send_sem=self.send_sems.at[k % POOL],
            recv_sem=self.recv_sems.at[k],
            device_id=(c, t, d),
            device_id_type=MESH,
        )

    def plan(self, ref, dev, dst=None):
        k = len(self.started)
        if k >= POOL:
            self.started[k - POOL][0].wait_send()
        self.started.append((self.copy(k, ref, ref if dst is None else dst, dev), dev))
        return k

    def start(self, k):
        self.started[k][0].start()

    def send(self, ref, dev, dst=None):
        k = self.plan(ref, dev, dst)
        self.start(k)
        return k

    def recv(self, k, ref):
        self.copy(k, ref, ref, self.started[k][1]).wait_recv()

    def finish(self):
        assert len(self.started) <= COPIES
        for copy, _ in self.started[-POOL:]:
            copy.wait_send()


def places():
    c, t, d = here()
    z, xl = c // 2, c % 2
    c1 = c + 1 - 2 * xl
    t1 = t + 1 - 2 * (t % 2)
    t2 = (t + 2) % 4
    t3 = (t1 + 2) % 4
    return types.SimpleNamespace(
        c=c, t=t, d=d, z=z, xl=xl, xo=1 - xl, c1=c1, t1=t1, t2=t2, t3=t3,
        P=(c1, t, d), Q=(c1, t2, d), C=(c, t1, d), R=(c, t2, d), D=(c, t3, d),
        Y={s: (c, t, (d + s) % 4) for s in SIDES},
        Z={s: ((c + 2 * s) % 8, t, d) for s in SIDES},
        yo={s: (d - s) % 4 for s in SIDES},
        zo={s: (z - s) % 4 for s in SIDES},
        y2=(d + 2) % 4, z2=(z + 2) % 4,
    )


def greet(m):
    barrier = pltpu.get_barrier_semaphore()
    others = [m.P, m.Q, m.C, m.R, m.D, m.Y[1], m.Y[-1], m.Z[1], m.Z[-1]]
    for dev in others:
        pl.semaphore_signal(barrier, inc=1, device_id=dev, device_id_type=MESH)
    pl.semaphore_wait(barrier, len(others))


def layer_kernel(
    hid, tgt, wq, wk, wv, wo, gain, order, turn_cos, turn_sin, block_cos, block_sin,
    out, loss_out,
    H, N, RH, W, acc, Q, KV, WO, AT, RA, num, peak, T, total, LB, row_cos, row_sin, ssem, rsem, lsem, osend, orecv, zsend, zrecv,
):
    m = places()
    net = Net(ssem, rsem)
    c, t, d = m.c, m.t, m.d
    local = [
        pltpu.make_async_copy(wq, W.at[c, d, :, pl.ds(0, 512)], lsem.at[0]),
        pltpu.make_async_copy(wk, W.at[c, d, :, pl.ds(512, 128)], lsem.at[1]),
        pltpu.make_async_copy(wv, W.at[c, d, :, pl.ds(640, 128)], lsem.at[2]),
        pltpu.make_async_copy(hid.at[0], H.at[t], lsem.at[3]),
    ]
    for cp in local:
        cp.start()
    later = pltpu.make_async_copy(tgt.at[0], T, lsem.at[4])
    later.start()
    turns = [
        pltpu.make_async_copy(turn_cos, row_cos, lsem.at[6]),
        pltpu.make_async_copy(turn_sin, row_sin, lsem.at[7]),
    ]
    for cp in turns:
        cp.start()
    own_wo = pltpu.make_async_copy(wo, WO.at[m.xl * 4 + d, pl.ds(m.z * 512, 512)], lsem.at[5])
    greet(m)
    for cp in local:
        cp.wait()

    def pair(z):
        return pl.ds(2 * z, 2)

    qa = {1: pl.ds(0, 32), -1: pl.ds(32, 32)}
    qb = {1: pl.ds(64, 32), -1: pl.ds(96, 32)}
    ha, hb = pl.ds(0, 64), pl.ds(64, 64)
    parts = 4
    rows = 256 // parts

    kX = [net.send(W.at[c, d, at], m.P) for at in (ha, hb)]
    kY1 = {s: net.send(W.at[c, d], m.Y[s]) for s in SIDES}
    kZ1 = {s: net.send(W.at[c, d], m.Z[s]) for s in SIDES}
    kH0 = [net.send(H.at[t, pl.ds(i * rows, rows)], m.P, RH.at[0, pl.ds(i * rows, rows)]) for i in range(parts)]
    kH1 = [net.send(H.at[t, pl.ds(256 + i * rows, rows)], m.Q, RH.at[1, pl.ds(i * rows, rows)]) for i in range(parts)]
    kC = net.send(H.at[t], m.C)

    mine = WO.at[m.xl * 4 + d]
    block = WO.at[m.xl * 4 + d, pl.ds(t * 512, 512)]

    def meet(k):
        return pltpu.make_async_remote_copy(
            src_ref=wo, dst_ref=block, send_sem=osend.at[4], recv_sem=orecv.at[4 + k],
            device_id=(c, m.z, d), device_id_type=MESH,
        )

    @pl.when(t == m.z)
    def _():
        own_wo.start()

    @pl.when(t != m.z)
    def _():
        meet(t).start()

    kY2, kZ2 = {}, {}
    for i, at in enumerate((ha, hb)):
        net.recv(kX[i], W.at[m.c1, d, at])
        for s in SIDES:
            kY2[s, i] = net.send(W.at[m.c1, d, at], m.Y[s])
            kZ2[s, i] = net.send(W.at[m.c1, d, at], m.Z[s])

    def relay(i):
        net.recv(kH0[i], RH.at[0, pl.ds(i * rows, rows)])
        a = net.send(RH.at[0, pl.ds(i * rows, rows)], m.Q, H.at[t, pl.ds(i * rows, rows)])
        net.recv(kH1[i], RH.at[1, pl.ds(i * rows, rows)])
        b = net.send(RH.at[1, pl.ds(i * rows, rows)], m.P, H.at[m.t2, pl.ds(256 + i * rows, rows)])
        return a, b

    far = []

    def landed(i):
        for k_, lo in ((kF[i][0], i * rows), (kF[i][1], 256 + i * rows)):
            net.recv(k_, H.at[m.t2, pl.ds(lo, rows)])
            far.append((net.send(H.at[m.t2, pl.ds(lo, rows)], m.C), lo))

    kF = []
    fY, fZ, kY3, kZ3, kY4, kZ4 = {}, {}, {}, {}, {}, {}
    for s in SIDES:
        net.recv(kY1[s], W.at[c, m.yo[s]])
        net.recv(kZ1[s], W.at[2 * m.zo[s] + m.xl, d])
    kF.append(relay(0))
    for s in SIDES:
        for i, at in enumerate((ha, hb)):
            net.recv(kY2[s, i], W.at[m.c1, m.yo[s], at])
        kY3[s] = net.send(W.at[pair(m.z), m.yo[s], qa[s]], m.Y[s])
        for i, at in enumerate((ha, hb)):
            net.recv(kZ2[s, i], W.at[2 * m.zo[s] + m.xo, d, at])
        kZ3[s] = net.send(W.at[pair(m.zo[s]), d, qb[s]], m.Z[s])
    for s in SIDES:
        for r in SIDES:
            kZ4[s, r] = net.send(W.at[pair(m.z), m.yo[s], ha], m.Z[r])
            kY4[s, r] = net.send(W.at[pair(m.zo[s]), d, hb], m.Y[r])

    kF += [relay(1), relay(2)]
    kY6, kZ6 = {}, {}
    for s in SIDES:
        net.recv(kY3[s], W.at[pair(m.z), m.y2, qa[s]])
        net.recv(kZ3[s], W.at[pair(m.z2), d, qb[s]])
    for r in SIDES:
        kZ6[r] = net.send(W.at[pair(m.z), m.y2, ha], m.Z[r])
        kY6[r] = net.send(W.at[pair(m.z2), d, hb], m.Y[r])
    for s in SIDES:
        fZ[s, "own"] = net.send(W.at[pair(m.zo[s]), d, qa[s]], m.Z[s])
        fY[s, "own"] = net.send(W.at[pair(m.z), m.yo[s], qb[s]], m.Y[s])
    kF.append(relay(3))
    for s in SIDES:
        for r in SIDES:
            net.recv(kZ4[s, r], W.at[pair(m.zo[r]), m.yo[s], ha])
            fZ[r, s] = net.send(W.at[pair(m.zo[r]), m.yo[s], qa[r]], m.Z[r])
            net.recv(kY4[s, r], W.at[pair(m.zo[s]), m.yo[r], hb])
            fY[r, s] = net.send(W.at[pair(m.zo[s]), m.yo[r], qb[r]], m.Y[r])
    landed(0)
    landed(1)
    landed(2)
    landed(3)
    for r in SIDES:
        net.recv(kZ6[r], W.at[pair(m.zo[r]), m.y2, ha])
        fZ[r, "far"] = net.send(W.at[pair(m.zo[r]), m.y2, qa[r]], m.Z[r])
        net.recv(kY6[r], W.at[pair(m.z2), m.yo[r], hb])
        fY[r, "far"] = net.send(W.at[pair(m.z2), m.yo[r], qb[r]], m.Y[r])
    turn = (m.z - t + 4) % 4

    def along(k, ref, s):
        return pltpu.make_async_remote_copy(
            src_ref=ref, dst_ref=ref, send_sem=zsend.at[k], recv_sem=zrecv.at[k],
            device_id=m.Z[s], device_id_type=MESH,
        )

    low = WO.at[m.xl * 4 + d, pl.ds(0, 1024)]
    high = WO.at[m.xl * 4 + d, pl.ds(1024, 1024)]

    @pl.when(turn == 0)
    def _():
        own_wo.wait()
        for k in range(4):
            @pl.when(k != t)
            def _(k=k):
                there = WO.at[m.xl * 4 + d, pl.ds(k * 512, 512)]
                pltpu.make_async_remote_copy(
                    src_ref=there, dst_ref=there, send_sem=osend.at[4], recv_sem=orecv.at[4 + k],
                    device_id=(c, m.z, d), device_id_type=MESH,
                ).wait_recv()

        along(0, low, 1).start()
        along(1, high, -1).start()
        along(4, high, 1).start()
        along(5, low, -1).start()

    def strip(xl, y, s=None):
        return WO.at[xl * 4 + y] if s is None else WO.at[xl * 4 + y, pl.ds(0 if s == 1 else 1024, 1024)]

    wo1 = {s: net.plan(mine, m.Y[s]) for s in SIDES}

    @pl.when(turn == 0)
    def _():
        for s in SIDES:
            net.start(wo1[s])

    net.recv(kC, H.at[m.t1])
    for k, lo in far:
        net.recv(k, H.at[m.t3, pl.ds(lo, rows)])


    step = 64

    def norm(i, carry):
        at = pl.ds(pl.multiple_of(i * step, step), step)
        total = jnp.zeros((step, 1), jnp.float32)
        for b in range(4):
            x = H[b, at, :].astype(jnp.float32)
            total = total + jnp.sum(x * x, axis=1, keepdims=True)
        scale = lax.rsqrt(total * (1.0 / MODEL_WIDTH) + 1e-05)
        for b in range(4):
            x = H[b, at, :].astype(jnp.float32)
            g = gain[:, b * 1024 : (b + 1) * 1024]
            N[b, at, :] = (x * scale * g).astype(jnp.bfloat16)
        return carry

    lax.fori_loop(0, 512 // step, norm, 0)

    def columns(zs, lo):
        cols = pl.ds(lo, 256)
        sums = None
        for z in zs:
            w = W[pair(z), :, :, cols].reshape(1024, 256)
            part = jnp.dot(N[z], w, preferred_element_type=jnp.float32)
            sums = part if sums is None else sums + part
        return sums

    for r in SIDES:
        net.recv(fY[r, "own"], W.at[pair(m.z), m.y2, qb[r]])
        for s in SIDES:
            net.recv(fY[r, s], W.at[pair(m.zo[s]), m.y2, qb[r]])
    acc[:, pl.ds(512, 256)] = columns((m.z, m.zo[1], m.zo[-1]), 512)

    for r in SIDES:
        net.recv(fZ[r, "own"], W.at[pair(m.z2), d, qa[r]])
        for s in SIDES:
            net.recv(fZ[r, s], W.at[pair(m.z2), m.yo[s], qa[r]])
        net.recv(fZ[r, "far"], W.at[pair(m.z2), m.y2, qa[r]])
        net.recv(fY[r, "far"], W.at[pair(m.z2), m.y2, qb[r]])
    acc[:, pl.ds(512, 256)] += columns((m.z2,), 512)
    for cp in turns:
        cp.wait()

    def rotate(heads):
        for s in range(2):
            where = order[2 * c + s]
            bc, bs = block_cos[pl.ds(where, 1), :], block_sin[pl.ds(where, 1), :]

            def rope(i, carry, s=s, bc=bc, bs=bs):
                rows_at = pl.ds(pl.multiple_of(i * step, step), step)
                at = pl.ds(pl.multiple_of(s * 256 + i * step, step), step)
                rc, rs = row_cos[rows_at, :], row_sin[rows_at, :]
                co = rc * bc - rs * bs
                si = rs * bc + rc * bs
                lane = lax.broadcasted_iota(jnp.int32, (step, 128), 1)
                si = jnp.where(lane < 64, -si, si)
                for h in heads:
                    x = acc[at, h * 128 : (h + 1) * 128]
                    y = (x * co + pltpu.roll(x, 64, 1) * si).astype(jnp.bfloat16)
                    if h < 4:
                        Q[h, at, :] = y
                    else:
                        KV[c, 0, at, :] = y
                        KV[c, 1, at, :] = acc[at, 640:768].astype(jnp.bfloat16)
                return carry

            lax.fori_loop(0, 256 // step, rope, 0)

    rotate((4,))
    @pl.when(turn == 1)
    def _():
        along(0, low, 1).wait_recv()
        along(2, low, 1).start()

    @pl.when(turn == 3)
    def _():
        along(1, high, -1).wait_recv()
        along(3, high, -1).start()

    kv0 = net.send(KV.at[c], m.P)
    kv1 = {s: net.send(KV.at[c], m.Z[s]) for s in SIDES}

    wo0 = {s: net.plan(strip(m.xl, d, s), m.P) for s in SIDES}

    @pl.when(turn == 0)
    def _():
        for s in SIDES:
            net.start(wo0[s])

    acc[:, pl.ds(0, 256)] = columns((m.z, m.zo[1], m.zo[-1], m.z2), 0)

    acc[:, pl.ds(256, 256)] = columns((m.z, m.zo[1], m.zo[-1], m.z2), 256)

    @pl.when(turn == 1)
    def _():
        along(4, high, 1).wait_recv()

    @pl.when(turn == 3)
    def _():
        along(5, low, -1).wait_recv()

    @pl.when(turn % 2 == 1)
    def _():
        for s in SIDES:
            net.start(wo1[s])
        for s in SIDES:
            net.start(wo0[s])

    rotate((0, 1, 2, 3))

    def bias(s, ctx, half):
        return jnp.where(order[2 * ctx + half] < order[2 * c + s], 0.0, NEG).astype(jnp.float32)

    ones = jnp.ones((512, 128), jnp.bfloat16)
    row = lax.broadcasted_iota(jnp.int32, (256, 256), 0)
    col = lax.broadcasted_iota(jnp.int32, (256, 256), 1)

    def tile(h, s, at, size, ctxs, first, lift):
        q = Q[h, at, :]
        pieces = []
        for ctx, lift_ in zip(ctxs, lift):
            x = lax.dot_general(q, KV[ctx, 0], (((1,), (1,)), ((), ())), preferred_element_type=jnp.float32)
            for half in range(2):
                y = x[:, half * 256 : (half + 1) * 256]
                if first and half == s:
                    y = jnp.where(row >= col, y, NEG)
                pieces.append((y, lift_[s][half]))
        top = None
        for y, b in pieces:
            e = jnp.maximum(y[:, :128], y[:, 128:]) + b
            top = e if top is None else jnp.maximum(top, e)
        new = jnp.broadcast_to(jnp.max(top, axis=1, keepdims=True), (size, 128))
        if not first:
            old = peak[h, at, :]
            new = jnp.maximum(old, new)
        level = new * SCALE
        p = []
        for y, b in pieces:
            down = b - level
            p.append(jnp.exp2(y * SCALE + jnp.concatenate([down, down], axis=1)).astype(jnp.bfloat16))
        part = None
        for i, ctx in enumerate(ctxs):
            value = jnp.concatenate([KV[ctx, 1], ones], axis=1)
            one = jnp.dot(jnp.concatenate(p[2 * i : 2 * i + 2], axis=1), value, preferred_element_type=jnp.float32)
            part = one if part is None else part + one
        if not first:
            factor = jnp.exp2((old - new) * SCALE)
            part = num[h, at, :] * jnp.concatenate([factor, factor], axis=1) + part
        return new, part

    def lifts(ctxs, first=False):
        out = []
        for ctx in ctxs:
            out.append([[jnp.float32(0.0) if first and s == half else bias(s, ctx, half) for half in range(2)] for s in range(2)])
        return out

    def tiles(h, ctxs, first, lift):
        size = 128 if len(ctxs) > 1 else 256
        out = []
        for s in range(2):
            for at in range(s * 256, (s + 1) * 256, size):
                at = pl.ds(at, size)
                out.append((at, tile(h, s, at, size, ctxs, first, lift)))
        return out

    def attend(ctxs, first=False, between=None):
        lift = lifts(ctxs, first)
        for h in range(4):
            if between is not None and h == 2:
                between()
            for at, (new, part) in tiles(h, ctxs, first, lift):
                peak[h, at, :], num[h, at, :] = new, part

    kv2, kv3, kv4, wo2, wo3, wo4 = {}, {}, {}, {}, {}, {}
    part_of = {1: 0, -1: 1}
    def to_z():
        net.recv(kv0, KV.at[m.c1])
        for s in SIDES:
            kv2[s] = net.send(KV.at[m.c1], m.Z[s])

        @pl.when(turn == 2)
        def _():
            along(2, low, 1).wait_recv()
            along(3, high, -1).wait_recv()
            for s in SIDES:
                net.start(wo1[s])
            for s in SIDES:
                net.start(wo0[s])

    attend((c,), True, to_z)

    for s in SIDES:
        there = 2 * m.zo[s] + m.xl
        net.recv(kv1[s], KV.at[there])
        kv3[s] = net.send(KV.at[there, part_of[s]], m.Z[s])
    attend([2 * m.zo[s] + m.xl for s in SIDES])
    for s in SIDES:
        wo3[s] = net.plan(strip(m.xl, m.yo[s], s), m.Y[s])

    def pass_on():
        for s in SIDES:
            net.recv(wo1[s], strip(m.xl, m.yo[s]))
            net.start(wo3[s])

    @pl.when(turn == 0)
    def _():
        pass_on()

    attend((m.c1,))
    for s in SIDES:
        there = 2 * m.zo[s] + m.xo
        net.recv(kv2[s], KV.at[there])
        kv4[s] = net.send(KV.at[there, part_of[s]], m.Z[s])
    for s in SIDES:
        net.recv(kv3[s], KV.at[2 * m.z2 + m.xl, part_of[s]])
    for r in SIDES:
        for s in SIDES:
            wo2[r, s] = net.plan(strip(m.xo, d, r), m.Y[s])

    def cross():
        for r in SIDES:
            net.recv(wo0[r], strip(m.xo, d, r))
            for s in SIDES:
                net.start(wo2[r, s])

    @pl.when(turn % 2 == 1)
    def _():
        pass_on()

    attend((2 * m.z2 + m.xl,))

    @pl.when(turn != 2)
    def _():
        cross()

    attend([2 * m.zo[s] + m.xo for s in SIDES])

    @pl.when(turn == 2)
    def _():
        pass_on()
        cross()


    for s in SIDES:
        net.recv(kv4[s], KV.at[2 * m.z2 + m.xo, part_of[s]])

    last = (2 * m.z2 + m.xo,)
    lift = lifts(last)
    top, bottom = pl.ds(0, 256), pl.ds(256, 256)
    kA = []
    for h in range(4):
        for at, (_, part) in tiles(h, last, False, lift):
            AT[t, h, at, :] = (part[:, :128] / part[:, 128:]).astype(jnp.bfloat16)
        ks = [net.send(AT.at[t, h, pl.ds(s * 256, 256)], (m.P, m.Q)[s], RA.at[s, h]) for s in range(2)]
        ks.append(net.send(AT.at[t, h], m.C))
        kA.append(ks)
    for s in SIDES:
        wo4[s] = net.plan(strip(m.xo, m.yo[s], s), m.Y[s])

    def hop(now):
        @pl.when(now)
        def _():
            for s in SIDES:
                net.recv(wo2[s, s], strip(m.xo, m.yo[s], s))
                net.start(wo4[s])

    hop(turn == 0)
    kR = []
    for h in range(4):
        net.recv(kA[h][0], RA.at[0, h])
        a = net.send(RA.at[0, h], m.Q, AT.at[t, h, top])
        net.recv(kA[h][1], RA.at[1, h])
        kR.append((a, net.send(RA.at[1, h], m.P, AT.at[m.t2, h, bottom])))
    soon = [[(m.xl, d), (m.xl, m.yo[1])], [(m.xl, m.yo[-1]), (m.xl, m.y2)], [(m.xo, d), (m.xo, m.yo[1])]]
    last_two = [(m.xo, m.yo[-1]), (m.xo, m.y2)]

    def product(bs, two):
        left = jnp.concatenate([AT[b, h] for b in bs for h in range(4)], axis=1)
        right = jnp.concatenate(
            [jnp.concatenate([WO[xl * 4 + y, pl.ds(b * 512, 512), :] for b in bs], axis=0) for xl, y in two], axis=1
        )
        return jnp.dot(left, right, preferred_element_type=jnp.float32)

    def project(bs, twos, first=False):
        for two in twos:
            part = product(bs, two)
            for i, (xl, y) in enumerate(two):
                cols = pl.ds(pl.multiple_of((xl * 4 + y) * 128, 128), 128)
                piece = part[:, i * 128 : (i + 1) * 128]
                if first:
                    total[:, cols] = piece
                else:
                    total[:, cols] += piece

    for h in range(4):
        net.recv(kA[h][2], AT.at[m.t1, h])
    project((t, m.t1), soon[:1], True)
    kD = []
    for h in range(4):
        net.recv(kR[h][0], AT.at[m.t2, h, top])
        net.recv(kR[h][1], AT.at[m.t2, h, bottom])
        kD.append(net.send(AT.at[m.t2, h], m.C))
        if h == 1:
            hop(turn % 2 == 1)
    hop(turn == 2)

    for s in SIDES:
        net.recv(wo3[s], strip(m.xl, m.y2, s))
    net.recv(wo2[-1, 1], strip(m.xo, m.yo[1], -1))
    net.recv(wo2[1, -1], strip(m.xo, m.yo[-1], 1))
    project((t, m.t1), soon[1:], True)
    project((m.t2,), soon)
    for h in range(4):
        net.recv(kD[h], AT.at[m.t3, h])
    project((m.t3,), soon)
    later.wait()

    def close(two, part):
        for xl, y in two:
            cols = pl.ds(pl.multiple_of((xl * 4 + y) * 128, 128), 128)
            for i in range(4):
                at = pl.ds(i * 128, 128)
                branch = total[at, cols].astype(jnp.bfloat16)
                out[at, cols] = branch
                gap = H[t, at, cols].astype(jnp.float32) + branch.astype(jnp.float32) - T[at, cols].astype(jnp.float32)
                sq = gap * gap
                fold = [sq[r * 8 : (r + 1) * 8] for r in range(16)]
                while len(fold) > 1:
                    fold = [a + b for a, b in zip(fold[::2], fold[1::2])]
                part = part + fold[0]
        return part

    part = jnp.zeros((8, 128), jnp.float32)
    for two in soon:
        part = close(two, part)
    for s in SIDES:
        net.recv(wo4[s], strip(m.xo, m.y2, s))
    rest = product((t, m.t1, m.t2, m.t3), last_two)
    for i, (xl, y) in enumerate(last_two):
        total[:, pl.ds(pl.multiple_of((xl * 4 + y) * 128, 128), 128)] = rest[:, i * 128 : (i + 1) * 128]
    part = close(last_two, part)
    rings = (
        (8, m.xl * 4 + t, lambda i: (2 * m.z + i // 4, i % 4, d)),
        (16, m.z * 4 + d, lambda i: (2 * (i // 4) + m.xl, t, i % 4)),
    )
    for number, (size, me, device) in enumerate(rings):
        LB[number, me] = part
        for j in range(1, size):
            pltpu.make_async_remote_copy(
                src_ref=LB.at[number, me], dst_ref=LB.at[number, me], send_sem=osend.at[5 + number],
                recv_sem=orecv.at[8 + number], device_id=device((me + j) % size), device_id_type=MESH,
            ).start()
        others = LB.at[number, pl.ds(0, size - 1)]
        pltpu.make_async_copy(others, others, orecv.at[8 + number]).wait()
        pltpu.make_async_copy(others, others, osend.at[5 + number]).wait()
        part = LB[number, 0]
        for j in range(1, size):
            part = part + LB[number, j]
    loss_out[0, 0] = jnp.sum(part) / (4 * 4096 * MODEL_WIDTH)
    net.finish()

    @pl.when(t != m.z)
    def _():
        meet(t).wait_send()

    for k, ref, s, when in ((0, low, 1, 0), (1, high, -1, 0), (4, high, 1, 0), (5, low, -1, 0), (2, low, 1, 1), (3, high, -1, 3)):
        @pl.when(turn == when)
        def _(k=k, ref=ref, s=s):
            along(k, ref, s).wait_send()


def tables():
    freqs = ROPE_BASE ** (-(np.arange(64) * 2.0) / HEAD_SIZE)
    freqs = np.concatenate([freqs, freqs])[None, :]
    rows, blocks = np.arange(256)[:, None] * freqs, np.arange(16)[:, None] * 256 * freqs
    return [f(x).astype(np.float32) for x in (rows, blocks) for f in (np.cos, np.sin)]


def on_device(hidden, target, gain, w_query, w_key, value_matrix, w_out, block_order):
    any_spec = pl.BlockSpec(memory_space=pl.ANY)
    vmem = pl.BlockSpec(memory_space=pltpu.VMEM)
    smem = pl.BlockSpec(memory_space=pltpu.SMEM)
    bf16, f32 = jnp.bfloat16, jnp.float32
    branch, loss = pl.pallas_call(
        layer_kernel,
        out_shape=(pltpu.VMEM((512, 1024), bf16), jax.ShapeDtypeStruct((1, 1), f32)),
        in_specs=[any_spec] * 6 + [vmem, smem, any_spec, any_spec, vmem, vmem],
        out_specs=(vmem, smem),
        scratch_shapes=[
            pltpu.VMEM((4, 512, 1024), bf16),
            pltpu.VMEM((4, 512, 1024), bf16),
            pltpu.VMEM((2, 256, 1024), bf16),
            pltpu.VMEM((8, 4, 128, 768), bf16),
            pltpu.VMEM((512, 768), f32),
            pltpu.VMEM((4, 512, 128), bf16),
            pltpu.VMEM((8, 2, 512, 128), bf16),
            pltpu.VMEM((8, 2048, 128), bf16),
            pltpu.VMEM((4, 4, 512, 128), bf16),
            pltpu.VMEM((2, 4, 256, 128), bf16),
            pltpu.VMEM((4, 512, 256), f32),
            pltpu.VMEM((4, 512, 128), f32),
            pltpu.VMEM((512, 1024), bf16),
            pltpu.VMEM((512, 1024), f32),
            pltpu.VMEM((2, 16, 8, 128), f32),
            pltpu.VMEM((256, 128), f32),
            pltpu.VMEM((256, 128), f32),
            pltpu.SemaphoreType.DMA((POOL,)),
            pltpu.SemaphoreType.DMA((COPIES,)),
            pltpu.SemaphoreType.DMA((8,)),
            pltpu.SemaphoreType.DMA((8,)),
            pltpu.SemaphoreType.DMA((10,)),
            pltpu.SemaphoreType.DMA((6,)),
            pltpu.SemaphoreType.DMA((6,)),
        ],
        compiler_params=pltpu.CompilerParams(
            collective_id=0, has_side_effects=True, vmem_limit_bytes=60 * MIB
        ),
        name="layer",
    )(hidden, target, w_query, w_key, value_matrix, w_out, gain[None, :], block_order, *(jnp.asarray(x) for x in tables()))
    return branch[None], loss.reshape(())


def solution(mesh):
    placed = (
        P("dp", "ctx", "tp"), P("dp", "ctx", "tp"), P(), P(("ctx", "dp"), "tp"), P(("ctx", "dp"), "tp"),
        P(("ctx", "dp"), "tp"), P("tp", ("ctx", "dp")), P(),
    )
    return jax.shard_map(
        on_device, mesh=mesh, in_specs=placed, out_specs=(P("dp", "ctx", "tp"), P()), check_vma=False
    )
```
